32 devices in a mesh: grp: 4 (over z), seq: 8 (over y, x, core).
Axes of the slice: x: 2, y: 2, z: 4, core: 2. Of those that a mesh axis runs over, the one named last changes fastest.
Arguments:
- latent: bfloat16 [4, 256, 32, 256], P('grp', 'seq'), may hold values from -6 to 6
- up_key: bfloat16 [4, 128, 256], replicated, may hold values from -0.5 to 0.5
- up_value: bfloat16 [4, 128, 256], replicated, may hold values from -0.5 to 0.5
- queries: bfloat16 [8, 64, 128], replicated, may hold values from -240 to 240, as said below
- lengths: int32 [8], replicated, may hold values from 1 to 1024
- block_dest: int32 [256], replicated, may hold values from 0 to 31, as said below
Outputs:
- decode_latent: bfloat16 [32, 4, 8, 32, 256], P(('grp', 'seq'))
- attended: float32 [8, 8192], replicated
The draws below stay inside these ranges and needn't reach their ends.
Inputs may be any that keep to these rules, and one draw needn't show every extreme that they name: `block_dest`: each aligned run of 32 entries (the blocks of one seq index in the prefill layout) names every decode device exactly once. `queries`: the new token's query entries, real-valued.
All inputs are finite; a program needn't handle non-finite values.
Results may differ from the reference program's by a relative error of at most 0.001.
Values may be sent and summed in bfloat16 or wider, within the bound.
A program may use at most 64 MiB of HBM per device.

```python
import jax
import jax.numpy as jnp
from jax import lax

Q_HEADS = 64
KV_HEADS = 8
HEAD_DIM = 128
RANK = 128
BATCH = 8
BT = 32
GROUPS = 4
DESTS = 32
BLOCKS = 256
S_MAX = 1024


def draw_queries(key, part):
    drawn = jnp.clip(jax.random.normal(key, (BATCH, Q_HEADS, HEAD_DIM), jnp.float32), -4.0, 4.0)
    return drawn.astype(jnp.bfloat16)


def draw_block_dest(key, part):
    shards = BLOCKS // DESTS
    subkeys = jax.random.split(jax.random.fold_in(key, 11), shards)
    orders = jax.vmap(lambda subkey: jax.random.permutation(subkey, DESTS))(subkeys)
    return orders.reshape(BLOCKS).astype(jnp.int32)


def place_ends(values, key, least, largest):
    place = [jax.random.randint(jax.random.fold_in(key, axis), (), 0, length) for axis, length in enumerate(values.shape)]
    main_axis = values.shape.index(max(values.shape))
    next_to = place[:main_axis] + [(place[main_axis] + 1) % values.shape[main_axis]] + place[main_axis + 1:]
    return values.at[tuple(place)].set(least).at[tuple(next_to)].set(largest)


def steps_of(stream_key, shape, cuts, smallest, high):
    loudness = 1.0
    for position, blocks in cuts:
        steps = jax.random.uniform(jax.random.fold_in(jax.random.fold_in(stream_key, 6), position), (blocks,), jnp.float32, smallest / len(cuts), high / len(cuts))
        loudness = loudness * jnp.repeat(jnp.exp(steps), shape[position] // blocks).reshape((-1,) + (1,) * (len(shape) - 1 - position))
    return loudness


def noise(key, extent, spread, bound, pieces=(), kind=jnp.bfloat16):
    entries = spread * jax.random.normal(key, extent, jnp.float32)
    if pieces:
        entries = entries * steps_of(key, extent, pieces, -0.22, 0.18)
    return jnp.clip(entries, -bound, bound).astype(kind)


def setup_inputs(seed: int = 0) -> dict:
    streams_of = jax.random.split(jax.random.key(seed), 7)
    latent = noise(streams_of[0], (GROUPS, BLOCKS, BT, 2 * RANK), 1.0, 6.0, ((0, 4), (1, 8)))
    up_key = noise(streams_of[1], (GROUPS, RANK, KV_HEADS // GROUPS * HEAD_DIM), RANK ** -0.5, 0.5)
    up_value = noise(streams_of[2], (GROUPS, RANK, KV_HEADS // GROUPS * HEAD_DIM), RANK ** -0.5, 0.5)
    queries = draw_queries(jax.random.fold_in(streams_of[6], 71), 0)
    lengths = place_ends(jax.random.randint(streams_of[4], (BATCH,), 1, S_MAX + 1), jax.random.fold_in(streams_of[4], 1), 1, S_MAX).astype(jnp.int32)
    block_dest = draw_block_dest(jax.random.fold_in(streams_of[6], 71), 0)
    return dict(latent=latent, up_key=up_key, up_value=up_value, queries=queries, lengths=lengths, block_dest=block_dest)


def reference(latent, up_key, up_value, queries, lengths, block_dest):
    shards = BLOCKS // DESTS
    table = block_dest.reshape(shards, DESTS)
    row_ids = jnp.broadcast_to(jnp.arange(shards, dtype=jnp.int32)[:, None], (shards, DESTS))
    col_ids = jnp.broadcast_to(jnp.arange(DESTS, dtype=jnp.int32)[None, :], (shards, DESTS))
    source_order = jnp.zeros((shards, DESTS), jnp.int32).at[row_ids, table].set(col_ids)
    global_ids = row_ids * DESTS + source_order
    picked = latent[:, global_ids.T]
    decode_latent = jnp.transpose(picked, (1, 0, 2, 3, 4))
    per_group = KV_HEADS // GROUPS
    per_kv = Q_HEADS // KV_HEADS
    scale = 1.0 / math_sqrt(HEAD_DIM)
    query_f = queries.astype(jnp.float32).reshape(BATCH, GROUPS, per_group, per_kv, HEAD_DIM)
    positions = jnp.arange(S_MAX, dtype=jnp.int32)
    valid = positions[None, :] < lengths[:, None]

    def one_group(index):
        lat = lax.dynamic_index_in_dim(latent, index, 0, keepdims=False).astype(jnp.float32)
        lat = lat.reshape(BATCH, S_MAX, 2 * RANK)
        key_map = lax.dynamic_index_in_dim(up_key, index, 0, keepdims=False).astype(jnp.float32)
        value_map = lax.dynamic_index_in_dim(up_value, index, 0, keepdims=False).astype(jnp.float32)
        keys = jnp.einsum('bsr,rc->bsc', lat[..., :RANK], key_map, precision=lax.Precision.HIGHEST)
        values = jnp.einsum('bsr,rc->bsc', lat[..., RANK:], value_map, precision=lax.Precision.HIGHEST)
        keys = keys.reshape(BATCH, S_MAX, per_group, HEAD_DIM)
        values = values.reshape(BATCH, S_MAX, per_group, HEAD_DIM)
        query_g = lax.dynamic_index_in_dim(query_f, index, 1, keepdims=False)
        scores = jnp.einsum('bkjd,bskd->bkjs', query_g, keys, precision=lax.Precision.HIGHEST) * scale
        live = valid[:, None, None, :]
        scores = jnp.where(live, scores, -1e+30)
        row_max = lax.optimization_barrier(jnp.max(scores, axis=-1, keepdims=True))
        weights = jnp.where(live, jnp.exp(scores - row_max), 0.0)
        totals = lax.optimization_barrier(jnp.sum(weights, axis=-1))
        summed = jnp.einsum('bkjs,bskd->bkjd', weights, values, precision=lax.Precision.HIGHEST)
        return summed / totals[..., None]
    outputs = lax.map(one_group, jnp.arange(GROUPS, dtype=jnp.int32))
    attended = jnp.transpose(outputs, (1, 0, 2, 3, 4)).reshape(BATCH, Q_HEADS * HEAD_DIM)
    return (decode_latent, attended)

def math_sqrt(value):
    return float(value) ** 0.5
```

```python
import functools

import jax
import jax.numpy as jnp
from jax import lax
from jax.experimental import pallas as pl
from jax.experimental.pallas import tpu as pltpu
from jax.sharding import PartitionSpec as P

MESH = pl.DeviceIdType.MESH
CORES = 2


def pieces(x, count):
    parts = []
    for _ in range(count - 1):
        part = x.astype(jnp.bfloat16)
        parts.append(part)
        x = x - part.astype(jnp.float32)
    parts.append(x.astype(jnp.bfloat16))
    return jnp.concatenate(parts, axis=0)


def dot_pieces(x, y, dims, count):
    rows = x.shape[0]
    out = lax.dot_general(pieces(x, count), y, (dims, ((), ())), preferred_element_type=jnp.float32)
    total = out[(count - 1) * rows :]
    for k in range(count - 2, -1, -1):
        total = total + out[k * rows : (k + 1) * rows]
    return total


def attend(per_group, per_kv, left, scale, lat, q, uk, uv):
    slots, block_len, width = lat.shape
    rank = width // 2
    heads, head_dim = q.shape
    tokens = slots * block_len
    query = q[...]

    def cols(m, k):
        return m[:, k * head_dim : (k + 1) * head_dim]

    def rows(m, k):
        return m[k * per_kv : (k + 1) * per_kv]

    key_map = uk[...]
    value_map = uv[...]
    absorbed = jnp.concatenate(
        [
            rows(
                lax.dot_general(query, cols(key_map, k), (((1,), (1,)), ((), ())), preferred_element_type=jnp.float32),
                k,
            )
            for k in range(per_group)
        ],
        axis=0,
    )
    key_lat = lat[:, :, :rank].reshape(tokens, rank)
    value_lat = lat[:, :, rank:].reshape(tokens, rank)
    scores = dot_pieces(absorbed, key_lat, ((1,), (1,)), 3) * scale
    live = lax.broadcasted_iota(jnp.int32, (heads, tokens), 1) < left
    scores = jnp.where(live, scores, -1e30)
    largest = jnp.max(scores, axis=1, keepdims=True)
    weights = jnp.where(live, jnp.exp(scores - largest), 0.0)
    total = jnp.sum(weights, axis=1, keepdims=True)
    some = jnp.where(total > 0.0, total, 1.0)
    mixed = dot_pieces(weights, value_lat, ((1,), (0,)), 3) / some
    values = jnp.concatenate(
        [rows(dot_pieces(mixed, cols(value_map, k), ((1,), (0,)), 3), k) for k in range(per_group)], axis=0
    )
    return values, jnp.where(total > 0.0, largest + jnp.log(some), -1e30)


def kernel(
    grps,
    seqs,
    per_seq,
    per_group,
    per_kv,
    dest_hbm,
    len_hbm,
    lat_hbm,
    q_hbm,
    uk_hbm,
    uv_hbm,
    recv_ref,
    att_ref,
    dest_s,
    len_s,
    lat_v,
    q_v,
    uk_v,
    uv_v,
    out_v,
    part_v,
    all_v,
    in_sems,
    send_a,
    recv_a,
    send_z,
    recv_z,
    send_p,
    recv_p,
    send_c,
    recv_c,
    plane_sem,
):
    n = grps * seqs
    chips = seqs // CORES
    group = lax.axis_index("grp")
    shard = lax.axis_index("seq")
    me = group * seqs + shard
    spot = shard // CORES
    core = lax.rem(shard, CORES)
    slots, block_len, width = lat_v.shape
    heads, head_dim = q_v.shape
    barrier = pltpu.get_barrier_semaphore()

    def signal(sem, there):
        pl.semaphore_signal(sem, inc=1, device_id=there, device_id_type=MESH)

    def send(src, dst, there, send_sem, recv_sem):
        pltpu.make_async_remote_copy(
            src_ref=src, dst_ref=dst, send_sem=send_sem, recv_sem=recv_sem, device_id=there, device_id_type=MESH
        ).start()

    def wait(some, sem):
        pltpu.make_async_copy(some, some, sem).wait()

    for j in range(1, grps):
        there = lax.rem(group + j, grps)
        for c in range(CORES):
            signal(barrier, (there, spot * CORES + c))

    @pl.loop(1, seqs)
    def _(k):
        signal(barrier, (group, lax.rem(shard + k, seqs)))

    sequence = shard // per_seq
    loads = [
        (dest_hbm, dest_s),
        (lat_hbm.at[0], lat_v),
        (q_hbm.at[sequence, pl.ds(pl.multiple_of(group * heads, heads), heads)], q_v),
        (uk_hbm.at[group], uk_v),
        (uv_hbm.at[group], uv_v),
        (len_hbm, len_s),
    ]
    loads = [pltpu.make_async_copy(src, dst, in_sems.at[i]) for i, (src, dst) in enumerate(loads)]
    for load in loads:
        load.start()

    loads[0].wait()
    lanes = pl.cdiv(n, 128) * 128
    lane = lax.broadcasted_iota(jnp.int32, (1, lanes), 1)

    def place(i, held):
        return jnp.where(lane == dest_s[shard * slots + i], i, held)

    unroll = min(slots, 32)
    source = lax.fori_loop(0, slots, place, jnp.zeros((1, lanes), jnp.int32), unroll=unroll)
    loads[1].wait()

    def pick(d, _):
        out_v[d] = lat_v[jnp.sum(jnp.where(lane == d, source, 0))]
        return 0

    lax.fori_loop(0, n, pick, 0, unroll=unroll)
    recv_ref[me] = out_v[me]

    pl.semaphore_wait(barrier, (grps - 1) * CORES + seqs - 1)
    for k in range(1, chips):
        signal(plane_sem, (group, lax.rem(spot + k, chips) * CORES + core))

    def block(to_group, to_shard):
        send(out_v.at[to_group * seqs + to_shard], recv_ref.at[me], (to_group, to_shard), send_a, recv_a)

    order = [1 + (j + grps // 2 - 1) % (grps - 1) for j in range(grps - 1)]
    for step in order:
        for c in range(CORES):
            block(lax.rem(group + step, grps), spot * CORES + lax.rem(core + c, CORES))

    @pl.loop(1, seqs)
    def _(k):
        block(group, lax.rem(shard + k, seqs))

    for load in loads[2:]:
        load.wait()
    left = len_s[sequence] - (shard - sequence * per_seq) * (slots * block_len)
    values, size = attend(per_group, per_kv, left, 1.0 / float(head_dim) ** 0.5, lat_v, q_v, uk_v, uv_v)
    part_v[0:heads, :] = values
    if per_seq > 1:
        part_v[heads : 2 * heads, :] = jnp.broadcast_to(size, (heads, head_dim))
    all_v[spot, core, group] = part_v[...]

    for k in range(1, grps):
        send(part_v, all_v.at[spot, core, group], (lax.rem(group + k, grps), shard), send_z, recv_z)

    pl.semaphore_wait(plane_sem, chips - 1)
    for step in order:

        @pl.loop(CORES, seqs)
        def _(k):
            block(lax.rem(group + step, grps), lax.rem(spot * CORES + k, seqs))

    wait(all_v.at[0, 0, pl.ds(0, grps - 1)], recv_z)
    own = all_v.at[spot, core]
    for k in range(1, chips):
        send(own, own, (group, lax.rem(spot + k, chips) * CORES + core), send_p, recv_p)
    wait(all_v.at[pl.ds(0, chips - 1), 0], recv_p)
    half = all_v.at[:, core]
    for c in range(1, CORES):
        send(half, half, (group, spot * CORES + lax.rem(core + c, CORES)), send_c, recv_c)
    wait(all_v.at[:, pl.ds(0, CORES - 1)], recv_c)

    batch = att_ref.shape[0]
    for g in range(grps):
        if per_seq == 1:
            held = all_v[:, :, g].reshape(batch, heads, head_dim)
        else:
            part = all_v[:, :, g].reshape(batch, per_seq, 2 * heads, head_dim)
            sizes = part[:, :, heads:]
            share = jnp.exp(sizes - jnp.max(sizes, axis=1, keepdims=True))
            held = jnp.sum(part[:, :, :heads] * share, axis=1) / jnp.sum(share, axis=1)
        held = jnp.swapaxes(held, 0, 1)
        for h in range(heads):
            at = (g * heads + h) * head_dim
            att_ref[:, at : at + head_dim] = held[h]

    wait(recv_ref.at[pl.ds(0, n - 1)], recv_a)
    wait(recv_ref.at[pl.ds(0, n - 1)], send_a)
    wait(all_v.at[0, 0, pl.ds(0, grps - 1)], send_z)
    wait(all_v.at[pl.ds(0, chips - 1), 0], send_p)
    wait(all_v.at[:, pl.ds(0, CORES - 1)], send_c)


def write_kernel(recv_ref, att_ref, latent_out, attended_out, sems):
    copies = [
        pltpu.make_async_copy(recv_ref, latent_out, sems.at[0]),
        pltpu.make_async_copy(att_ref, attended_out, sems.at[1]),
    ]
    for copy in copies:
        copy.start()
    for copy in copies:
        copy.wait()


def body(grps, seqs, latent, up_key, up_value, queries, lengths, block_dest):
    groups, rank, maps = up_key.shape
    slots, block_len, width = latent.shape[1:]
    batch, q_heads, head_dim = queries.shape
    per_group = maps // head_dim
    heads = q_heads // groups
    per_kv = heads // per_group
    n = grps * seqs
    blk_seq = block_dest.shape[0] // batch
    per_seq = blk_seq // slots
    assert per_seq * slots == blk_seq and n == slots and groups == grps and seqs % CORES == 0
    part_rows = heads if per_seq == 1 else 2 * heads
    anywhere = pl.BlockSpec(memory_space=pl.ANY)
    vmem = pl.BlockSpec(memory_space=pltpu.VMEM)
    dma = pltpu.SemaphoreType.DMA
    received, attended = pl.pallas_call(
        functools.partial(kernel, grps, seqs, per_seq, per_group, per_kv),
        out_shape=(
            pltpu.VMEM((n, block_len, width), latent.dtype),
            pltpu.VMEM((batch, q_heads * head_dim), jnp.float32),
        ),
        in_specs=[anywhere] * 6,
        out_specs=(vmem, vmem),
        scratch_shapes=[
            pltpu.SMEM(block_dest.shape, jnp.int32),
            pltpu.SMEM(lengths.shape, jnp.int32),
            pltpu.VMEM((slots, block_len, width), latent.dtype),
            pltpu.VMEM((heads, head_dim), queries.dtype),
            pltpu.VMEM((rank, maps), up_key.dtype),
            pltpu.VMEM((rank, maps), up_value.dtype),
            pltpu.VMEM((n, block_len, width), latent.dtype),
            pltpu.VMEM((part_rows, head_dim), jnp.float32),
            pltpu.VMEM((seqs // CORES, CORES, grps, part_rows, head_dim), jnp.float32),
            dma((6,)),
        ]
        + [dma] * 8
        + [pltpu.SemaphoreType.REGULAR],
        compiler_params=pltpu.CompilerParams(collective_id=0, has_side_effects=True),
        name="exchange",
    )(block_dest, lengths, latent, queries, up_key, up_value)
    decode_latent, attended = pl.pallas_call(
        write_kernel,
        out_shape=(
            jax.ShapeDtypeStruct(received.shape, received.dtype),
            jax.ShapeDtypeStruct(attended.shape, attended.dtype),
        ),
        in_specs=[anywhere] * 2,
        out_specs=(anywhere, anywhere),
        scratch_shapes=[dma((2,))],
        name="write_out",
    )(pltpu.with_memory_space_constraint(received, pltpu.VMEM), pltpu.with_memory_space_constraint(attended, pltpu.VMEM))
    return (decode_latent.reshape(1, groups, seqs, block_len, width), attended)


def solution(mesh):
    return jax.shard_map(
        functools.partial(body, mesh.shape["grp"], mesh.shape["seq"]),
        mesh=mesh,
        in_specs=(P("grp", "seq", None, None), P(), P(), P(), P(), P()),
        out_specs=(P(("grp", "seq"), None, None, None, None), P()),
        check_vma=False,
    )
```

```python
import functools
import math

import jax
import jax.numpy as jnp
from jax import lax
from jax.experimental import pallas as pl
from jax.experimental.pallas import tpu as pltpu
from jax.sharding import PartitionSpec as P

MESH = pl.DeviceIdType.MESH
CORES = 2


def pieces(x, count):
    parts = []
    for _ in range(count - 1):
        part = x.astype(jnp.bfloat16)
        parts.append(part)
        x = x - part.astype(jnp.float32)
    parts.append(x.astype(jnp.bfloat16))
    return jnp.concatenate(parts, axis=0)


def dot_pieces(x, y, dims, count):
    rows = x.shape[0]
    out = lax.dot_general(pieces(x, count), y, (dims, ((), ())), preferred_element_type=jnp.float32)
    total = out[(count - 1) * rows :]
    for k in range(count - 2, -1, -1):
        total = total + out[k * rows : (k + 1) * rows]
    return total


def attend(per_group, per_kv, left, scale, lat, q, uk, uv):
    slots, block_len, width = lat.shape
    rank = width // 2
    heads, head_dim = q.shape
    tokens = slots * block_len
    query = q[...]

    def cols(m, k):
        return m[:, k * head_dim : (k + 1) * head_dim]

    def rows(m, k):
        return m[k * per_kv : (k + 1) * per_kv]

    key_map = uk[...]
    value_map = uv[...]
    absorbed = jnp.concatenate(
        [
            rows(
                lax.dot_general(query, cols(key_map, k), (((1,), (1,)), ((), ())), preferred_element_type=jnp.float32),
                k,
            )
            for k in range(per_group)
        ],
        axis=0,
    )
    key_lat = lat[:, :, :rank].reshape(tokens, rank)
    value_lat = lat[:, :, rank:].reshape(tokens, rank)
    scores = dot_pieces(absorbed, key_lat, ((1,), (1,)), 3) * scale
    live = lax.broadcasted_iota(jnp.int32, (heads, tokens), 1) < left
    scores = jnp.where(live, scores, -1e30)
    largest = jnp.max(scores, axis=1, keepdims=True)
    weights = jnp.where(live, jnp.exp(scores - largest), 0.0)
    total = jnp.sum(weights, axis=1, keepdims=True)
    some = jnp.where(total > 0.0, total, 1.0)
    mixed = dot_pieces(weights, value_lat, ((1,), (0,)), 3) / some
    values = jnp.concatenate(
        [rows(dot_pieces(mixed, cols(value_map, k), ((1,), (0,)), 3), k) for k in range(per_group)], axis=0
    )
    return values, jnp.where(total > 0.0, largest + jnp.log(some), -1e30)


def kernel(
    grps,
    seqs,
    per_seq,
    per_group,
    per_kv,
    dest_hbm,
    len_hbm,
    lat_hbm,
    q_hbm,
    uk_hbm,
    uv_hbm,
    recv_ref,
    att_ref,
    dest_s,
    len_s,
    lat_v,
    q_v,
    uk_v,
    uv_v,
    out_v,
    part_v,
    all_v,
    in_sems,
    send_a,
    recv_near,
    recv_far,
    send_z,
    recv_z,
    send_p,
    recv_p,
    send_c,
    recv_c,
    send_b,
    recv_b,
    plane_sem,
    line_sem,
    all_sem,
    go_sem,
):
    n = grps * seqs
    chips = seqs // CORES
    half = grps // 2
    group = lax.axis_index("grp")
    shard = lax.axis_index("seq")
    me = group * seqs + shard
    spot = shard // CORES
    core = lax.rem(shard, CORES)
    side = group // half
    first_far = (1 - side) * half
    leads = core == CORES - 1
    last = (group == grps - 1) & (spot == chips - 1)
    bits = [lax.rem(spot // 2**b, 2) for b in range(chips.bit_length() - 1)]
    slots, block_len, width = lat_v.shape
    heads, head_dim = q_v.shape
    barrier = pltpu.get_barrier_semaphore()

    def signal(sem, there):
        pl.semaphore_signal(sem, inc=1, device_id=there, device_id_type=MESH)

    def send(src, dst, there, send_sem, recv_sem):
        pltpu.make_async_remote_copy(
            src_ref=src, dst_ref=dst, send_sem=send_sem, recv_sem=recv_sem, device_id=there, device_id_type=MESH
        ).start()

    def wait(some, sem):
        pltpu.make_async_copy(some, some, sem).wait()

    def bits_in(v):
        return sum(bit for b, bit in enumerate(bits) if v >> b & 1)

    def count(of):
        total = 1
        for bit in bits:
            total = total * of(bit)
        return total

    sequence = shard // per_seq
    loads = [
        (dest_hbm, dest_s),
        (lat_hbm.at[0], lat_v),
        (q_hbm.at[sequence, pl.ds(pl.multiple_of(group * heads, heads), heads)], q_v),
        (uk_hbm.at[group], uk_v),
        (uv_hbm.at[group], uv_v),
        (len_hbm, len_s),
    ]
    loads = [pltpu.make_async_copy(src, dst, in_sems.at[i]) for i, (src, dst) in enumerate(loads)]
    for load in loads[:2]:
        load.start()

    with jax.named_scope("sig"):
        for c in range(1, CORES):
            signal(barrier, (group, spot * CORES + lax.rem(core + c, CORES)))
        for v in range(chips):

            @pl.when(bits_in(v) == 0)
            def _():
                @pl.loop(group + (1 if v == 0 else 0), grps)
                def _(g):
                    for c in range(CORES):
                        signal(barrier, (g, (spot + v) * CORES + c))

    for load in loads[2:]:
        load.start()
    with jax.named_scope("w_bar"):
        pl.semaphore_wait(barrier, ((group + 1) * count(lambda bit: 1 + bit) - 1) * CORES + CORES - 1)

    with jax.named_scope("sig2"):
        for v in range(1, chips):

            @pl.when(bits_in(v) == bin(v).count("1"))
            def _():
                signal(plane_sem, (group, (spot - v) * CORES + core))

        @pl.when(group == half)
        def _():
            @pl.loop(0, half)
            def _(g):
                signal(line_sem, (g, shard))

        @pl.when(last)
        def _():
            @pl.loop(0, grps * chips - 1)
            def _(k):
                signal(all_sem, (k // chips, lax.rem(k, chips) * CORES + core))

    with jax.named_scope("w_dest"):
        loads[0].wait()
    lanes = pl.cdiv(n, 128) * 128
    lane = lax.broadcasted_iota(jnp.int32, (1, lanes), 1)

    def place(i, held):
        return jnp.where(lane == dest_s[shard * slots + i], i, held)

    unroll = min(slots, 32)
    source = lax.fori_loop(0, slots, place, jnp.zeros((1, lanes), jnp.int32), unroll=unroll)
    with jax.named_scope("w_lat"):
        loads[1].wait()

    def pick(d, _):
        out_v[d] = lat_v[jnp.sum(jnp.where(lane == d, source, 0))]
        return 0

    with jax.named_scope("pick"):
        lax.fori_loop(0, n, pick, 0, unroll=unroll)
        recv_ref[me] = out_v[me]

    def block(to_group, to_shard, recv_sem):
        send(out_v.at[to_group * seqs + to_shard], recv_ref.at[me], (to_group, to_shard), send_a, recv_sem)

    def turn(table, k):
        if table is None:
            return lax.rem(spot + k, chips)
        return sum(
            row[k] * math.prod(bit if a >> b & 1 else 1 - bit for b, bit in enumerate(bits))
            for a, row in enumerate(table)
            if row[k]
        )

    upper_turns = ((0, 1, 2, 3), (0, 1, 3, 2), (0, 2, 1, 3), (1, 0, 2, 3)) if chips == 4 else None
    lower_turns = ((0, 1, 2, 3), (1, 0, 3, 2), (2, 0, 1, 3), (3, 1, 0, 2)) if chips == 4 else None

    def far_blocks(turns, j, first, end):
        for k in range(first, end):
            to_spot = turn(turns, k)
            for c in range(CORES):
                block(first_far + j, to_spot * CORES + lax.rem(core + c, CORES), recv_far)

    def near_blocks(lowest, highest):
        @pl.loop(lowest, highest)
        def _(g):
            @pl.loop(0, seqs)
            def _(k):
                block(g, lax.rem(shard + k, seqs), recv_near)

    @pl.when(side == 1)
    def _():
        far_blocks(upper_turns, 0, 0, 1)

    for load in loads[2:]:
        load.wait()
    with jax.named_scope("attend"):
        left = len_s[sequence] - (shard - sequence * per_seq) * (slots * block_len)
        values, size = attend(per_group, per_kv, left, 1.0 / float(head_dim) ** 0.5, lat_v, q_v, uk_v, uv_v)
        part_v[0:heads, :] = values
        if per_seq > 1:
            part_v[heads : 2 * heads, :] = jnp.broadcast_to(size, (heads, head_dim))

    @pl.when(core < CORES - 1)
    def _():
        send(part_v, all_v.at[spot, group, core], (group, spot * CORES + CORES - 1), send_c, recv_c)

    @pl.when(leads)
    def _():
        all_v[spot, group, core] = part_v[...]

    @pl.when(side == 0)
    def _():
        with jax.named_scope("w_line"):
            pl.semaphore_wait(line_sem, 1)
        far_blocks(lower_turns, 0, 0, 1)

    with jax.named_scope("w_plane"):

        @pl.when(spot < chips - 1)
        def _():
            pl.semaphore_wait(plane_sem, count(lambda bit: 2 - bit) - 1)

    @pl.loop(1, seqs)
    def _(k):
        block(group, lax.rem(shard + k, seqs), recv_near)

    def along_line(g):
        both = all_v.at[spot, group]
        send(both, both, (g, shard), send_z, recv_z.at[group])

    def over_plane(g):
        both = all_v.at[spot, g]
        for k in range(1, chips):
            send(both, both, (group, lax.rem(spot + k, chips) * CORES + core), send_p, recv_p)

    def release():
        @pl.when(leads)
        def _():
            for c in range(CORES - 1):
                signal(go_sem, (group, spot * CORES + c))

        @pl.when(core < CORES - 1)
        def _():
            pl.semaphore_wait(go_sem, 1)

    @pl.when(leads)
    def _():
        with jax.named_scope("w_part"):
            wait(all_v.at[0, 0, pl.ds(0, CORES - 1)], recv_c)

        @pl.loop(0, group)
        def _(g):
            along_line(g)

    @pl.when(side == 1)
    def _():
        release()
        for j in range(half):
            far_blocks(upper_turns, j, 0 if j else 1, chips)

    with jax.named_scope("w_all"):

        @pl.when(jnp.logical_not(last))
        def _():
            pl.semaphore_wait(all_sem, 1)

    @pl.when(leads)
    def _():
        @pl.loop(group + 1, grps)
        def _(g):
            along_line(g)

        over_plane(group)

    @pl.when(side == 0)
    def _():
        release()
        for j in range(half):
            far_blocks(lower_turns, j, 1, chips)
        for j in range(1, half):
            far_blocks(lower_turns, j, 0, 1)

    near_blocks(side * half, group)
    near_blocks(group + 1, (side + 1) * half)

    @pl.when(leads)
    def _():
        for k in range(1, grps):
            for g in (group - k, group + k):

                @pl.when((g >= 0) & (g < grps))
                def _():
                    with jax.named_scope("w_z"):
                        wait(all_v.at[0, 0], recv_z.at[g])
                    over_plane(g)

        with jax.named_scope("w_p"):
            wait(all_v.at[pl.ds(0, chips - 1)], recv_p)
        for c in range(CORES - 1):
            send(all_v, all_v, (group, spot * CORES + c), send_b, recv_b)

    @pl.when(core < CORES - 1)
    def _():
        with jax.named_scope("w_c"):
            wait(all_v, recv_b)

    batch = att_ref.shape[0]
    with jax.named_scope("att"):
        for g in range(grps):
            if per_seq == 1:
                held = all_v[:, g].reshape(batch, heads, head_dim)
            else:
                part = all_v[:, g].reshape(batch, per_seq, 2 * heads, head_dim)
                sizes = part[:, :, heads:]
                share = jnp.exp(sizes - jnp.max(sizes, axis=1, keepdims=True))
                held = jnp.sum(part[:, :, :heads] * share, axis=1) / jnp.sum(share, axis=1)
            held = jnp.swapaxes(held, 0, 1)
            for h in range(heads):
                at = (g * heads + h) * head_dim
                att_ref[:, at : at + head_dim] = held[h]

    with jax.named_scope("w_near"):
        wait(recv_ref.at[pl.ds(0, n // 2 - 1)], recv_near)
    with jax.named_scope("w_far"):
        wait(recv_ref.at[pl.ds(0, n // 2)], recv_far)
    with jax.named_scope("w_send"):
        wait(recv_ref.at[pl.ds(0, n - 1)], send_a)

    @pl.when(leads)
    def _():
        wait(all_v.at[0, pl.ds(0, grps - 1)], send_z)
        wait(all_v.at[pl.ds(0, chips - 1)], send_p)
        for c in range(CORES - 1):
            wait(all_v, send_b)

    @pl.when(core < CORES - 1)
    def _():
        wait(part_v, send_c)


def write_kernel(recv_ref, att_ref, latent_out, attended_out, sems):
    copies = [
        pltpu.make_async_copy(recv_ref, latent_out, sems.at[0]),
        pltpu.make_async_copy(att_ref, attended_out, sems.at[1]),
    ]
    for copy in copies:
        copy.start()
    for copy in copies:
        copy.wait()


def body(grps, seqs, latent, up_key, up_value, queries, lengths, block_dest):
    groups, rank, maps = up_key.shape
    slots, block_len, width = latent.shape[1:]
    batch, q_heads, head_dim = queries.shape
    per_group = maps // head_dim
    heads = q_heads // groups
    per_kv = heads // per_group
    n = grps * seqs
    blk_seq = block_dest.shape[0] // batch
    per_seq = blk_seq // slots
    assert per_seq * slots == blk_seq and n == slots and groups == grps
    assert grps % 2 == 0 and seqs % CORES == 0 and seqs // CORES & (seqs // CORES - 1) == 0
    part_rows = heads if per_seq == 1 else 2 * heads
    anywhere = pl.BlockSpec(memory_space=pl.ANY)
    vmem = pl.BlockSpec(memory_space=pltpu.VMEM)
    dma = pltpu.SemaphoreType.DMA
    received, attended = pl.pallas_call(
        functools.partial(kernel, grps, seqs, per_seq, per_group, per_kv),
        out_shape=(
            pltpu.VMEM((n, block_len, width), latent.dtype),
            pltpu.VMEM((batch, q_heads * head_dim), jnp.float32),
        ),
        in_specs=[anywhere] * 6,
        out_specs=(vmem, vmem),
        scratch_shapes=[
            pltpu.SMEM(block_dest.shape, jnp.int32),
            pltpu.SMEM(lengths.shape, jnp.int32),
            pltpu.VMEM((slots, block_len, width), latent.dtype),
            pltpu.VMEM((heads, head_dim), queries.dtype),
            pltpu.VMEM((rank, maps), up_key.dtype),
            pltpu.VMEM((rank, maps), up_value.dtype),
            pltpu.VMEM((n, block_len, width), latent.dtype),
            pltpu.VMEM((part_rows, head_dim), jnp.float32),
            pltpu.VMEM((seqs // CORES, grps, CORES, part_rows, head_dim), jnp.float32),
            dma((6,)),
        ]
        + [dma] * 4
        + [dma((grps,))]
        + [dma] * 6
        + [pltpu.SemaphoreType.REGULAR] * 4,
        compiler_params=pltpu.CompilerParams(collective_id=0, has_side_effects=True),
        name="exchange",
    )(block_dest, lengths, latent, queries, up_key, up_value)
    decode_latent, attended = pl.pallas_call(
        write_kernel,
        out_shape=(
            jax.ShapeDtypeStruct(received.shape, received.dtype),
            jax.ShapeDtypeStruct(attended.shape, attended.dtype),
        ),
        in_specs=[anywhere] * 2,
        out_specs=(anywhere, anywhere),
        scratch_shapes=[dma((2,))],
        name="write_out",
    )(pltpu.with_memory_space_constraint(received, pltpu.VMEM), pltpu.with_memory_space_constraint(attended, pltpu.VMEM))
    return (decode_latent.reshape(1, groups, seqs, block_len, width), attended)


def solution(mesh):
    return jax.shard_map(
        functools.partial(body, mesh.shape["grp"], mesh.shape["seq"]),
        mesh=mesh,
        in_specs=(P("grp", "seq", None, None), P(), P(), P(), P(), P()),
        out_specs=(P(("grp", "seq"), None, None, None, None), P()),
        check_vma=False,
    )
```

```python
import functools
import math

import jax
import jax.numpy as jnp
from jax import lax
from jax.experimental import pallas as pl
from jax.experimental.pallas import tpu as pltpu
from jax.sharding import PartitionSpec as P

MESH = pl.DeviceIdType.MESH
CORES = 2


def pieces(x, count):
    parts = []
    for _ in range(count - 1):
        part = x.astype(jnp.bfloat16)
        parts.append(part)
        x = x - part.astype(jnp.float32)
    parts.append(x.astype(jnp.bfloat16))
    return jnp.concatenate(parts, axis=0)


def dot_pieces(x, y, dims, count):
    rows = x.shape[0]
    out = lax.dot_general(pieces(x, count), y, (dims, ((), ())), preferred_element_type=jnp.float32)
    total = out[(count - 1) * rows :]
    for k in range(count - 2, -1, -1):
        total = total + out[k * rows : (k + 1) * rows]
    return total


def attend(per_group, per_kv, left, scale, lat, q, uk, uv):
    slots, block_len, width = lat.shape
    rank = width // 2
    heads, head_dim = q.shape
    tokens = slots * block_len
    query = q[...]

    def cols(m, k):
        return m[:, k * head_dim : (k + 1) * head_dim]

    def rows(m, k):
        return m[k * per_kv : (k + 1) * per_kv]

    key_map = uk[...]
    value_map = uv[...]
    absorbed = jnp.concatenate(
        [
            rows(
                lax.dot_general(query, cols(key_map, k), (((1,), (1,)), ((), ())), preferred_element_type=jnp.float32),
                k,
            )
            for k in range(per_group)
        ],
        axis=0,
    )
    key_lat = lat[:, :, :rank].reshape(tokens, rank)
    value_lat = lat[:, :, rank:].reshape(tokens, rank)
    scores = dot_pieces(absorbed, key_lat, ((1,), (1,)), 3) * scale
    live = lax.broadcasted_iota(jnp.int32, (heads, tokens), 1) < left
    scores = jnp.where(live, scores, -1e30)
    largest = jnp.max(scores, axis=1, keepdims=True)
    weights = jnp.where(live, jnp.exp(scores - largest), 0.0)
    total = jnp.sum(weights, axis=1, keepdims=True)
    some = jnp.where(total > 0.0, total, 1.0)
    mixed = dot_pieces(weights, value_lat, ((1,), (0,)), 3) / some
    values = jnp.concatenate(
        [rows(dot_pieces(mixed, cols(value_map, k), ((1,), (0,)), 3), k) for k in range(per_group)], axis=0
    )
    return values, jnp.where(total > 0.0, largest + jnp.log(some), -1e30)


def kernel(
    grps,
    seqs,
    per_seq,
    per_group,
    per_kv,
    dest_hbm,
    len_hbm,
    lat_hbm,
    q_hbm,
    uk_hbm,
    uv_hbm,
    recv_ref,
    att_ref,
    dest_s,
    len_s,
    from_s,
    lat_v,
    q_v,
    uk_v,
    uv_v,
    out_v,
    part_v,
    all_v,
    in_sems,
    send_a,
    recv_near,
    recv_far,
    send_z,
    recv_z,
    send_p,
    recv_p,
    send_c,
    recv_c,
    send_b,
    recv_b,
    plane_sem,
    line_sem,
    all_sem,
    go_sem,
    top_sem,
    mid_sem,
):
    n = grps * seqs
    chips = seqs // CORES
    half = grps // 2
    group = lax.axis_index("grp")
    shard = lax.axis_index("seq")
    me = group * seqs + shard
    spot = shard // CORES
    core = lax.rem(shard, CORES)
    side = group // half
    first_far = (1 - side) * half
    leads = core == CORES - 1
    last = (group == grps - 1) & (spot == chips - 1)
    bits = [lax.rem(spot // 2**b, 2) for b in range(chips.bit_length() - 1)]
    slots, block_len, width = lat_v.shape
    heads, head_dim = q_v.shape
    barrier = pltpu.get_barrier_semaphore()

    def signal(sem, there):
        pl.semaphore_signal(sem, inc=1, device_id=there, device_id_type=MESH)

    def send(src, dst, there, send_sem, recv_sem):
        pltpu.make_async_remote_copy(
            src_ref=src, dst_ref=dst, send_sem=send_sem, recv_sem=recv_sem, device_id=there, device_id_type=MESH
        ).start()

    def wait(some, sem):
        pltpu.make_async_copy(some, some, sem).wait()

    def bits_in(v):
        return sum(bit for b, bit in enumerate(bits) if v >> b & 1)

    def count(of):
        total = 1
        for bit in bits:
            total = total * of(bit)
        return total

    sequence = shard // per_seq
    loads = [
        (dest_hbm, dest_s),
        (lat_hbm.at[0], lat_v),
        (q_hbm.at[sequence, pl.ds(pl.multiple_of(group * heads, heads), heads)], q_v),
        (uk_hbm.at[group], uk_v),
        (uv_hbm.at[group], uv_v),
        (len_hbm, len_s),
    ]
    loads = [pltpu.make_async_copy(src, dst, in_sems.at[i]) for i, (src, dst) in enumerate(loads)]
    for load in loads[:2]:
        load.start()

    with jax.named_scope("sig"):
        for c in range(1, CORES):
            signal(barrier, (group, spot * CORES + lax.rem(core + c, CORES)))
        for v in range(chips):

            @pl.when(bits_in(v) == 0)
            def _():
                @pl.loop(group + (1 if v == 0 else 0), grps)
                def _(g):
                    for c in range(CORES):
                        signal(barrier, (g, (spot + v) * CORES + c))

    for load in loads[2:]:
        load.start()
    with jax.named_scope("w_bar"):
        pl.semaphore_wait(barrier, ((group + 1) * count(lambda bit: 1 + bit) - 1) * CORES + CORES - 1)

    with jax.named_scope("sig2"):
        for v in range(1, chips):

            @pl.when(bits_in(v) == bin(v).count("1"))
            def _():
                signal(plane_sem, (group, (spot - v) * CORES + core))

        @pl.when(group == half)
        def _():
            @pl.loop(0, half)
            def _(g):
                signal(line_sem, (g, shard))

        @pl.when(group == grps - 1)
        def _():
            @pl.loop(0, grps - 1)
            def _(g):
                signal(top_sem, (g, shard))

        @pl.when((group == half) & (spot == chips - 1))
        def _():
            @pl.loop(0, half * chips)
            def _(k):
                signal(mid_sem, (k // chips, lax.rem(k, chips) * CORES + core))

        @pl.when(last)
        def _():
            @pl.loop(0, grps * chips - 1)
            def _(k):
                signal(all_sem, (k // chips, lax.rem(k, chips) * CORES + core))

    with jax.named_scope("w_dest"):
        loads[0].wait()
    lanes = pl.cdiv(n, 128) * 128
    lane = lax.broadcasted_iota(jnp.int32, (1, lanes), 1)

    def place(i, held):
        return jnp.where(lane == dest_s[shard * slots + i], i, held)

    unroll = min(slots, 32)
    source = lax.fori_loop(0, slots, place, jnp.zeros((1, lanes), jnp.int32), unroll=unroll)

    def find(d, _):
        from_s[d] = jnp.sum(jnp.where(lane == d, source, 0))
        return 0

    lax.fori_loop(0, n, find, 0, unroll=unroll)
    with jax.named_scope("w_lat"):
        loads[1].wait()

    def pick(d, _):
        out_v[d] = lat_v[from_s[d]]
        return 0

    with jax.named_scope("pick"):
        lax.fori_loop(0, n, pick, 0, unroll=unroll)
        recv_ref[me] = out_v[me]

    def block(to_group, to_shard, recv_sem):
        send(out_v.at[to_group * seqs + to_shard], recv_ref.at[me], (to_group, to_shard), send_a, recv_sem)

    def turn(table, k):
        if table is None:
            return lax.rem(spot + k, chips)
        return sum(
            row[k] * math.prod(bit if a >> b & 1 else 1 - bit for b, bit in enumerate(bits))
            for a, row in enumerate(table)
            if row[k]
        )

    if chips == 4:
        upper_turns = ((0, 1, 2, 3), (0, 1, 3, 2), (0, 2, 1, 3), (1, 0, 2, 3))
        lower_turns = ((0, 1, 2, 3), (1, 0, 3, 2), (2, 3, 0, 1), (3, 0, 1, 2))
    else:
        upper_turns = lower_turns = None
    ahead = (spot > 0) & (core < CORES - 1) & (chips == 4)

    def far_blocks(turns, j, first, end):
        for k in range(first, end):
            to_spot = turn(turns, k)
            for c in range(CORES):
                block(first_far + j, to_spot * CORES + lax.rem(core + c, CORES), recv_far)

    def near_blocks(lowest, highest):
        @pl.loop(lowest, highest)
        def _(g):
            @pl.loop(0, seqs)
            def _(k):
                block(g, lax.rem(shard + k, seqs), recv_near)

    @pl.when(side == 1)
    def _():
        far_blocks(upper_turns, 0, 0, 1)

        @pl.when(ahead)
        def _():
            far_blocks(upper_turns, 0, 1, 2)

    for load in loads[2:]:
        load.wait()
    with jax.named_scope("attend"):
        left = len_s[sequence] - (shard - sequence * per_seq) * (slots * block_len)
        values, size = attend(per_group, per_kv, left, 1.0 / float(head_dim) ** 0.5, lat_v, q_v, uk_v, uv_v)
        part_v[0:heads, :] = values
        if per_seq > 1:
            part_v[heads : 2 * heads, :] = jnp.broadcast_to(size, (heads, head_dim))

    @pl.when(core < CORES - 1)
    def _():
        send(part_v, all_v.at[spot, group, core], (group, spot * CORES + CORES - 1), send_c, recv_c)

    @pl.when(leads)
    def _():
        all_v[spot, group, core] = part_v[...]

    @pl.when(side == 0)
    def _():
        with jax.named_scope("w_line"):
            pl.semaphore_wait(line_sem, 1)
        far_blocks(lower_turns, 0, 0, 1)

    with jax.named_scope("w_plane"):

        @pl.when(spot < chips - 1)
        def _():
            pl.semaphore_wait(plane_sem, count(lambda bit: 2 - bit) - 1)

    @pl.loop(1, seqs)
    def _(k):
        block(group, lax.rem(shard + k, seqs), recv_near)

    def along_line(g):
        both = all_v.at[spot, group]
        send(both, both, (g, shard), send_z, recv_z.at[group])

    def over_plane(g):
        both = all_v.at[spot, g]
        for k in range(1, chips):
            send(both, both, (group, lax.rem(spot + k, chips) * CORES + core), send_p, recv_p)

    def release():
        @pl.when(leads)
        def _():
            for c in range(CORES - 1):
                signal(go_sem, (group, spot * CORES + c))

        @pl.when(core < CORES - 1)
        def _():
            pl.semaphore_wait(go_sem, 1)

    @pl.when(leads)
    def _():
        with jax.named_scope("w_part"):
            wait(all_v.at[0, 0, pl.ds(0, CORES - 1)], recv_c)

        @pl.loop(0, group)
        def _(g):
            along_line(g)

    def parts_up():
        with jax.named_scope("w_top"):

            @pl.when(group < grps - 1)
            def _():
                pl.semaphore_wait(top_sem, 1)

        @pl.when(leads)
        def _():
            @pl.loop(group + 1, grps)
            def _(g):
                along_line(g)

    @pl.when(side == 1)
    def _():
        release()

        @pl.when(jnp.logical_not(ahead))
        def _():
            far_blocks(upper_turns, 0, 1, 2)

        far_blocks(upper_turns, 0, 2, chips)
        for j in range(1, half):
            far_blocks(lower_turns, j, 1, chips)
        for j in range(1, half):
            far_blocks(lower_turns, j, 0, 1)

    @pl.when(side == 0)
    def _():
        parts_up()
        release()
        with jax.named_scope("w_mid"):
            pl.semaphore_wait(mid_sem, 1)
        far_blocks(lower_turns, 0, 1, chips)

    with jax.named_scope("w_all"):

        @pl.when(jnp.logical_not(last))
        def _():
            pl.semaphore_wait(all_sem, 1)

    @pl.when(side == 0)
    def _():
        for j in range(1, half):
            far_blocks(lower_turns, j, 1, chips)
        for j in range(1, half):
            far_blocks(lower_turns, j, 0, 1)

    @pl.when(side == 1)
    def _():
        parts_up()

    @pl.when(leads)
    def _():
        over_plane(group)

    near_blocks(side * half, group)
    near_blocks(group + 1, (side + 1) * half)

    @pl.when(leads)
    def _():
        for k in range(1, grps):
            for g in (group - k, group + k):

                @pl.when((g >= 0) & (g < grps))
                def _():
                    with jax.named_scope("w_z"):
                        wait(all_v.at[0, 0], recv_z.at[g])
                    over_plane(g)

        with jax.named_scope("w_p"):
            wait(all_v.at[pl.ds(0, chips - 1)], recv_p)
        for c in range(CORES - 1):
            send(all_v, all_v, (group, spot * CORES + c), send_b, recv_b)

    @pl.when(core < CORES - 1)
    def _():
        with jax.named_scope("w_c"):
            wait(all_v, recv_b)

    batch = att_ref.shape[0]
    with jax.named_scope("att"):
        for g in range(grps):
            if per_seq == 1:
                held = all_v[:, g].reshape(batch, heads, head_dim)
            else:
                part = all_v[:, g].reshape(batch, per_seq, 2 * heads, head_dim)
                sizes = part[:, :, heads:]
                share = jnp.exp(sizes - jnp.max(sizes, axis=1, keepdims=True))
                held = jnp.sum(part[:, :, :heads] * share, axis=1) / jnp.sum(share, axis=1)
            held = jnp.swapaxes(held, 0, 1)
            for h in range(heads):
                at = (g * heads + h) * head_dim
                att_ref[:, at : at + head_dim] = held[h]

    with jax.named_scope("w_send"):
        wait(recv_ref.at[pl.ds(0, n - 1)], send_a)

    @pl.when(leads)
    def _():
        wait(all_v.at[0, pl.ds(0, grps - 1)], send_z)
        wait(all_v.at[pl.ds(0, chips - 1)], send_p)
        for c in range(CORES - 1):
            wait(all_v, send_b)

    @pl.when(core < CORES - 1)
    def _():
        wait(part_v, send_c)

    with jax.named_scope("w_near"):
        wait(recv_ref.at[pl.ds(0, n // 2 - 1)], recv_near)
    with jax.named_scope("w_far"):
        wait(recv_ref.at[pl.ds(0, n // 2)], recv_far)


def write_kernel(recv_ref, att_ref, latent_out, attended_out, sems):
    copies = [
        pltpu.make_async_copy(recv_ref, latent_out, sems.at[0]),
        pltpu.make_async_copy(att_ref, attended_out, sems.at[1]),
    ]
    for copy in copies:
        copy.start()
    for copy in copies:
        copy.wait()


def body(grps, seqs, latent, up_key, up_value, queries, lengths, block_dest):
    groups, rank, maps = up_key.shape
    slots, block_len, width = latent.shape[1:]
    batch, q_heads, head_dim = queries.shape
    per_group = maps // head_dim
    heads = q_heads // groups
    per_kv = heads // per_group
    n = grps * seqs
    blk_seq = block_dest.shape[0] // batch
    per_seq = blk_seq // slots
    assert per_seq * slots == blk_seq and n == slots and groups == grps
    assert grps % 2 == 0 and seqs % CORES == 0 and seqs // CORES & (seqs // CORES - 1) == 0
    part_rows = heads if per_seq == 1 else 2 * heads
    anywhere = pl.BlockSpec(memory_space=pl.ANY)
    vmem = pl.BlockSpec(memory_space=pltpu.VMEM)
    dma = pltpu.SemaphoreType.DMA
    received, attended = pl.pallas_call(
        functools.partial(kernel, grps, seqs, per_seq, per_group, per_kv),
        out_shape=(
            pltpu.VMEM((n, block_len, width), latent.dtype),
            pltpu.VMEM((batch, q_heads * head_dim), jnp.float32),
        ),
        in_specs=[anywhere] * 6,
        out_specs=(vmem, vmem),
        scratch_shapes=[
            pltpu.SMEM(block_dest.shape, jnp.int32),
            pltpu.SMEM(lengths.shape, jnp.int32),
            pltpu.SMEM((n,), jnp.int32),
            pltpu.VMEM((slots, block_len, width), latent.dtype),
            pltpu.VMEM((heads, head_dim), queries.dtype),
            pltpu.VMEM((rank, maps), up_key.dtype),
            pltpu.VMEM((rank, maps), up_value.dtype),
            pltpu.VMEM((n, block_len, width), latent.dtype),
            pltpu.VMEM((part_rows, head_dim), jnp.float32),
            pltpu.VMEM((seqs // CORES, grps, CORES, part_rows, head_dim), jnp.float32),
            dma((6,)),
        ]
        + [dma] * 4
        + [dma((grps,))]
        + [dma] * 6
        + [pltpu.SemaphoreType.REGULAR] * 6,
        compiler_params=pltpu.CompilerParams(collective_id=0, has_side_effects=True),
        name="exchange",
    )(block_dest, lengths, latent, queries, up_key, up_value)
    decode_latent, attended = pl.pallas_call(
        write_kernel,
        out_shape=(
            jax.ShapeDtypeStruct(received.shape, received.dtype),
            jax.ShapeDtypeStruct(attended.shape, attended.dtype),
        ),
        in_specs=[anywhere] * 2,
        out_specs=(anywhere, anywhere),
        scratch_shapes=[dma((2,))],
        name="write_out",
    )(pltpu.with_memory_space_constraint(received, pltpu.VMEM), pltpu.with_memory_space_constraint(attended, pltpu.VMEM))
    return (decode_latent.reshape(1, groups, seqs, block_len, width), attended)


def solution(mesh):
    return jax.shard_map(
        functools.partial(body, mesh.shape["grp"], mesh.shape["seq"]),
        mesh=mesh,
        in_specs=(P("grp", "seq", None, None), P(), P(), P(), P(), P()),
        out_specs=(P(("grp", "seq"), None, None, None, None), P()),
        check_vma=False,
    )
```

```python
import functools
import math

import jax
import jax.numpy as jnp
from jax import lax
from jax.experimental import pallas as pl
from jax.experimental.pallas import tpu as pltpu
from jax.sharding import PartitionSpec as P

MESH = pl.DeviceIdType.MESH
CORES = 2


def pieces(x, count):
    parts = []
    for _ in range(count - 1):
        part = x.astype(jnp.bfloat16)
        parts.append(part)
        x = x - part.astype(jnp.float32)
    parts.append(x.astype(jnp.bfloat16))
    return jnp.concatenate(parts, axis=0)


def dot_pieces(x, y, dims, count):
    rows = x.shape[0]
    out = lax.dot_general(pieces(x, count), y, (dims, ((), ())), preferred_element_type=jnp.float32)
    total = out[(count - 1) * rows :]
    for k in range(count - 2, -1, -1):
        total = total + out[k * rows : (k + 1) * rows]
    return total


def attend(per_group, per_kv, left, scale, lat, q, uk, uv):
    slots, block_len, width = lat.shape
    rank = width // 2
    heads, head_dim = q.shape
    tokens = slots * block_len
    query = q[...]

    def cols(m, k):
        return m[:, k * head_dim : (k + 1) * head_dim]

    def rows(m, k):
        return m[k * per_kv : (k + 1) * per_kv]

    key_map = uk[...]
    value_map = uv[...]
    absorbed = jnp.concatenate(
        [
            rows(
                lax.dot_general(query, cols(key_map, k), (((1,), (1,)), ((), ())), preferred_element_type=jnp.float32),
                k,
            )
            for k in range(per_group)
        ],
        axis=0,
    )
    key_lat = lat[:, :, :rank].reshape(tokens, rank)
    value_lat = lat[:, :, rank:].reshape(tokens, rank)
    scores = dot_pieces(absorbed, key_lat, ((1,), (1,)), 3) * scale
    live = lax.broadcasted_iota(jnp.int32, (heads, tokens), 1) < left
    scores = jnp.where(live, scores, -1e30)
    largest = jnp.max(scores, axis=1, keepdims=True)
    weights = jnp.where(live, jnp.exp(scores - largest), 0.0)
    total = jnp.sum(weights, axis=1, keepdims=True)
    some = jnp.where(total > 0.0, total, 1.0)
    mixed = dot_pieces(weights, value_lat, ((1,), (0,)), 3) / some
    values = jnp.concatenate(
        [rows(dot_pieces(mixed, cols(value_map, k), ((1,), (0,)), 3), k) for k in range(per_group)], axis=0
    )
    return values, jnp.where(total > 0.0, largest + jnp.log(some), -1e30)


def kernel(
    grps,
    seqs,
    per_seq,
    per_group,
    per_kv,
    dest_hbm,
    len_hbm,
    lat_hbm,
    q_hbm,
    uk_hbm,
    uv_hbm,
    recv_ref,
    att_ref,
    dest_s,
    len_s,
    from_s,
    lat_v,
    q_v,
    uk_v,
    uv_v,
    out_v,
    part_v,
    all_v,
    in_sems,
    send_a,
    recv_near,
    recv_far,
    send_z,
    recv_z,
    send_p,
    recv_p,
    send_c,
    recv_c,
    send_b,
    recv_b,
    plane_sem,
    line_sem,
    all_sem,
    go_sem,
    top_sem,
    mid_sem,
):
    n = grps * seqs
    chips = seqs // CORES
    half = grps // 2
    group = lax.axis_index("grp")
    shard = lax.axis_index("seq")
    me = group * seqs + shard
    spot = shard // CORES
    core = lax.rem(shard, CORES)
    side = group // half
    first_far = (1 - side) * half
    leads = core == CORES - 1
    last = (group == grps - 1) & (spot == chips - 1)
    bits = [lax.rem(spot // 2**b, 2) for b in range(chips.bit_length() - 1)]
    slots, block_len, width = lat_v.shape
    heads, head_dim = q_v.shape
    barrier = pltpu.get_barrier_semaphore()

    def signal(sem, there):
        pl.semaphore_signal(sem, inc=1, device_id=there, device_id_type=MESH)

    def send(src, dst, there, send_sem, recv_sem):
        pltpu.make_async_remote_copy(
            src_ref=src, dst_ref=dst, send_sem=send_sem, recv_sem=recv_sem, device_id=there, device_id_type=MESH
        ).start()

    def wait(some, sem):
        pltpu.make_async_copy(some, some, sem).wait()

    def bits_in(v):
        return sum(bit for b, bit in enumerate(bits) if v >> b & 1)

    def count(of):
        total = 1
        for bit in bits:
            total = total * of(bit)
        return total

    sequence = shard // per_seq
    loads = [
        (dest_hbm, dest_s),
        (lat_hbm.at[0], lat_v),
        (q_hbm.at[sequence, pl.ds(pl.multiple_of(group * heads, heads), heads)], q_v),
        (uk_hbm.at[group], uk_v),
        (uv_hbm.at[group], uv_v),
        (len_hbm, len_s),
    ]
    loads = [pltpu.make_async_copy(src, dst, in_sems.at[i]) for i, (src, dst) in enumerate(loads)]
    for load in loads[:2]:
        load.start()

    with jax.named_scope("sig"):
        for c in range(1, CORES):
            signal(barrier, (group, spot * CORES + lax.rem(core + c, CORES)))
        for v in range(chips):

            @pl.when(bits_in(v) == 0)
            def _():
                @pl.loop(group + (1 if v == 0 else 0), grps)
                def _(g):
                    for c in range(CORES):
                        signal(barrier, (g, (spot + v) * CORES + c))

    for load in loads[2:]:
        load.start()
    with jax.named_scope("w_bar"):
        pl.semaphore_wait(barrier, ((group + 1) * count(lambda bit: 1 + bit) - 1) * CORES + CORES - 1)

    with jax.named_scope("sig2"):
        for v in range(1, chips):

            @pl.when(bits_in(v) == bin(v).count("1"))
            def _():
                signal(plane_sem, (group, (spot - v) * CORES + core))

        @pl.when(group == half)
        def _():
            @pl.loop(0, half)
            def _(g):
                signal(line_sem, (g, shard))

        @pl.when(group == grps - 1)
        def _():
            @pl.loop(0, grps - 1)
            def _(g):
                signal(top_sem, (g, shard))

        @pl.when((group == half) & (spot == chips - 1))
        def _():
            @pl.loop(0, half * chips)
            def _(k):
                signal(mid_sem, (k // chips, lax.rem(k, chips) * CORES + core))

        @pl.when(last)
        def _():
            @pl.loop(0, grps * chips - 1)
            def _(k):
                signal(all_sem, (k // chips, lax.rem(k, chips) * CORES + core))

    with jax.named_scope("w_dest"):
        loads[0].wait()
    lanes = pl.cdiv(n, 128) * 128
    lane = lax.broadcasted_iota(jnp.int32, (1, lanes), 1)

    def place(i, held):
        return jnp.where(lane == dest_s[shard * slots + i], i, held)

    unroll = min(slots, 32)
    source = lax.fori_loop(0, slots, place, jnp.zeros((1, lanes), jnp.int32), unroll=unroll)

    def find(d, _):
        from_s[d] = jnp.sum(jnp.where(lane == d, source, 0))
        return 0

    lax.fori_loop(0, n, find, 0, unroll=unroll)
    with jax.named_scope("w_lat"):
        loads[1].wait()

    def pick(d, _):
        out_v[d] = lat_v[from_s[d]]
        return 0

    with jax.named_scope("pick"):
        lax.fori_loop(0, n, pick, 0, unroll=unroll)
        recv_ref[me] = out_v[me]

    def block(to_group, to_shard, recv_sem):
        send(out_v.at[to_group * seqs + to_shard], recv_ref.at[me], (to_group, to_shard), send_a, recv_sem)

    def turn(table, k):
        if table is None:
            return lax.rem(spot + k, chips)
        return sum(
            row[k] * math.prod(bit if a >> b & 1 else 1 - bit for b, bit in enumerate(bits))
            for a, row in enumerate(table)
            if row[k]
        )

    if chips == 4:
        upper_turns = ((0, 1, 2, 3), (0, 1, 3, 2), (0, 2, 1, 3), (1, 0, 2, 3))
        lower_turns = ((0, 1, 2, 3), (1, 0, 3, 2), (2, 3, 0, 1), (3, 0, 1, 2))
    else:
        upper_turns = lower_turns = None
    ahead_own = (spot == 0) & (core < CORES - 1)
    ahead = (spot > 0) & (core < CORES - 1) & (chips == 4)

    def far_blocks(turns, j, first, end):
        for k in range(first, end):
            to_spot = turn(turns, k)
            for c in range(CORES):
                block(first_far + j, to_spot * CORES + lax.rem(core + c, CORES), recv_far)

    def near_blocks(lowest, highest):
        @pl.loop(lowest, highest)
        def _(g):
            @pl.loop(0, seqs)
            def _(k):
                block(g, lax.rem(shard + k, seqs), recv_near)

    @pl.when(side == 1)
    def _():
        far_blocks(upper_turns, 0, 0, 1)

        @pl.when(ahead)
        def _():
            far_blocks(upper_turns, 0, 1, 2)

        @pl.when(ahead_own)
        def _():
            for j in range(1, half):
                far_blocks(lower_turns, j, 0, 1)

    for load in loads[2:]:
        load.wait()
    with jax.named_scope("attend"):
        left = len_s[sequence] - (shard - sequence * per_seq) * (slots * block_len)
        values, size = attend(per_group, per_kv, left, 1.0 / float(head_dim) ** 0.5, lat_v, q_v, uk_v, uv_v)
        part_v[0:heads, :] = values
        if per_seq > 1:
            part_v[heads : 2 * heads, :] = jnp.broadcast_to(size, (heads, head_dim))

    @pl.when(core < CORES - 1)
    def _():
        send(part_v, all_v.at[spot, group, core], (group, spot * CORES + CORES - 1), send_c, recv_c)

    @pl.when(leads)
    def _():
        all_v[spot, group, core] = part_v[...]

    @pl.when(side == 0)
    def _():
        with jax.named_scope("w_line"):
            pl.semaphore_wait(line_sem, 1)
        far_blocks(lower_turns, 0, 0, 1)

    with jax.named_scope("w_plane"):

        @pl.when(spot < chips - 1)
        def _():
            pl.semaphore_wait(plane_sem, count(lambda bit: 2 - bit) - 1)

    @pl.loop(1, seqs)
    def _(k):
        block(group, lax.rem(shard + k, seqs), recv_near)

    def along_line(g):
        both = all_v.at[spot, group]
        send(both, both, (g, shard), send_z, recv_z.at[group])

    def over_plane(g):
        both = all_v.at[spot, g]
        for k in range(1, chips):
            send(both, both, (group, lax.rem(spot + k, chips) * CORES + core), send_p, recv_p)

    def release():
        @pl.when(leads)
        def _():
            for c in range(CORES - 1):
                signal(go_sem, (group, spot * CORES + c))

        @pl.when(core < CORES - 1)
        def _():
            pl.semaphore_wait(go_sem, 1)

    @pl.when(core < CORES - 1)
    def _():
        near_blocks(side * half, group)

    @pl.when(leads)
    def _():
        with jax.named_scope("w_part"):
            wait(all_v.at[0, 0, pl.ds(0, CORES - 1)], recv_c)

        @pl.loop(0, group)
        def _(g):
            along_line(g)

        near_blocks(side * half, group)

    def parts_up():
        with jax.named_scope("w_top"):

            @pl.when(group < grps - 1)
            def _():
                pl.semaphore_wait(top_sem, 1)

        @pl.when(leads)
        def _():
            @pl.loop(group + 1, grps)
            def _(g):
                along_line(g)

    @pl.when(side == 1)
    def _():
        release()

        @pl.when(jnp.logical_not(ahead))
        def _():
            far_blocks(upper_turns, 0, 1, 2)

        far_blocks(upper_turns, 0, 2, chips)
        for j in range(1, half):
            far_blocks(lower_turns, j, 1, chips)

        @pl.when(jnp.logical_not(ahead_own))
        def _():
            for j in range(1, half):
                far_blocks(lower_turns, j, 0, 1)

    @pl.when(side == 0)
    def _():
        parts_up()
        release()
        with jax.named_scope("w_mid"):
            pl.semaphore_wait(mid_sem, 1)
        near_blocks(group + 1, half)
        far_blocks(lower_turns, 0, 1, chips)

    with jax.named_scope("w_all"):

        @pl.when(jnp.logical_not(last))
        def _():
            pl.semaphore_wait(all_sem, 1)

    @pl.when(side == 0)
    def _():
        for j in range(1, half):
            far_blocks(lower_turns, j, 1, chips)
        for j in range(1, half):
            far_blocks(lower_turns, j, 0, 1)

    @pl.when(side == 1)
    def _():
        parts_up()
        near_blocks(group + 1, grps)

    @pl.when(leads)
    def _():
        over_plane(group)


    @pl.when(leads)
    def _():
        for k in range(1, grps):
            for g in (group - k, group + k):

                @pl.when((g >= 0) & (g < grps))
                def _():
                    with jax.named_scope("w_z"):
                        wait(all_v.at[0, 0], recv_z.at[g])
                    over_plane(g)

        with jax.named_scope("w_p"):
            wait(all_v.at[pl.ds(0, chips - 1)], recv_p)
        for c in range(CORES - 1):
            send(all_v, all_v, (group, spot * CORES + c), send_b, recv_b)

    @pl.when(core < CORES - 1)
    def _():
        with jax.named_scope("w_c"):
            wait(all_v, recv_b)

    batch = att_ref.shape[0]
    with jax.named_scope("att"):
        for g in range(grps):
            if per_seq == 1:
                held = all_v[:, g].reshape(batch, heads, head_dim)
            else:
                part = all_v[:, g].reshape(batch, per_seq, 2 * heads, head_dim)
                sizes = part[:, :, heads:]
                share = jnp.exp(sizes - jnp.max(sizes, axis=1, keepdims=True))
                held = jnp.sum(part[:, :, :heads] * share, axis=1) / jnp.sum(share, axis=1)
            held = jnp.swapaxes(held, 0, 1)
            for h in range(heads):
                at = (g * heads + h) * head_dim
                att_ref[:, at : at + head_dim] = held[h]

    with jax.named_scope("w_send"):
        wait(recv_ref.at[pl.ds(0, n - 1)], send_a)

    @pl.when(leads)
    def _():
        wait(all_v.at[0, pl.ds(0, grps - 1)], send_z)
        wait(all_v.at[pl.ds(0, chips - 1)], send_p)
        for c in range(CORES - 1):
            wait(all_v, send_b)

    @pl.when(core < CORES - 1)
    def _():
        wait(part_v, send_c)

    with jax.named_scope("w_near"):
        wait(recv_ref.at[pl.ds(0, n // 2 - 1)], recv_near)
    with jax.named_scope("w_far"):
        wait(recv_ref.at[pl.ds(0, n // 2)], recv_far)


def write_kernel(recv_ref, att_ref, latent_out, attended_out, sems):
    copies = [
        pltpu.make_async_copy(recv_ref, latent_out, sems.at[0]),
        pltpu.make_async_copy(att_ref, attended_out, sems.at[1]),
    ]
    for copy in copies:
        copy.start()
    for copy in copies:
        copy.wait()


def body(grps, seqs, latent, up_key, up_value, queries, lengths, block_dest):
    groups, rank, maps = up_key.shape
    slots, block_len, width = latent.shape[1:]
    batch, q_heads, head_dim = queries.shape
    per_group = maps // head_dim
    heads = q_heads // groups
    per_kv = heads // per_group
    n = grps * seqs
    blk_seq = block_dest.shape[0] // batch
    per_seq = blk_seq // slots
    assert per_seq * slots == blk_seq and n == slots and groups == grps
    assert grps % 2 == 0 and seqs % CORES == 0 and seqs // CORES & (seqs // CORES - 1) == 0
    part_rows = heads if per_seq == 1 else 2 * heads
    anywhere = pl.BlockSpec(memory_space=pl.ANY)
    vmem = pl.BlockSpec(memory_space=pltpu.VMEM)
    dma = pltpu.SemaphoreType.DMA
    received, attended = pl.pallas_call(
        functools.partial(kernel, grps, seqs, per_seq, per_group, per_kv),
        out_shape=(
            pltpu.VMEM((n, block_len, width), latent.dtype),
            pltpu.VMEM((batch, q_heads * head_dim), jnp.float32),
        ),
        in_specs=[anywhere] * 6,
        out_specs=(vmem, vmem),
        scratch_shapes=[
            pltpu.SMEM(block_dest.shape, jnp.int32),
            pltpu.SMEM(lengths.shape, jnp.int32),
            pltpu.SMEM((n,), jnp.int32),
            pltpu.VMEM((slots, block_len, width), latent.dtype),
            pltpu.VMEM((heads, head_dim), queries.dtype),
            pltpu.VMEM((rank, maps), up_key.dtype),
            pltpu.VMEM((rank, maps), up_value.dtype),
            pltpu.VMEM((n, block_len, width), latent.dtype),
            pltpu.VMEM((part_rows, head_dim), jnp.float32),
            pltpu.VMEM((seqs // CORES, grps, CORES, part_rows, head_dim), jnp.float32),
            dma((6,)),
        ]
        + [dma] * 4
        + [dma((grps,))]
        + [dma] * 6
        + [pltpu.SemaphoreType.REGULAR] * 6,
        compiler_params=pltpu.CompilerParams(collective_id=0, has_side_effects=True),
        name="exchange",
    )(block_dest, lengths, latent, queries, up_key, up_value)
    decode_latent, attended = pl.pallas_call(
        write_kernel,
        out_shape=(
            jax.ShapeDtypeStruct(received.shape, received.dtype),
            jax.ShapeDtypeStruct(attended.shape, attended.dtype),
        ),
        in_specs=[anywhere] * 2,
        out_specs=(anywhere, anywhere),
        scratch_shapes=[dma((2,))],
        name="write_out",
    )(pltpu.with_memory_space_constraint(received, pltpu.VMEM), pltpu.with_memory_space_constraint(attended, pltpu.VMEM))
    return (decode_latent.reshape(1, groups, seqs, block_len, width), attended)


def solution(mesh):
    return jax.shard_map(
        functools.partial(body, mesh.shape["grp"], mesh.shape["seq"]),
        mesh=mesh,
        in_specs=(P("grp", "seq", None, None), P(), P(), P(), P(), P()),
        out_specs=(P(("grp", "seq"), None, None, None, None), P()),
        check_vma=False,
    )
```

```python
import functools
import math

import jax
import jax.numpy as jnp
from jax import lax
from jax.experimental import pallas as pl
from jax.experimental.pallas import tpu as pltpu
from jax.sharding import PartitionSpec as P

MESH = pl.DeviceIdType.MESH
CORES = 2


def pieces(x, count):
    parts = []
    for _ in range(count - 1):
        part = x.astype(jnp.bfloat16)
        parts.append(part)
        x = x - part.astype(jnp.float32)
    parts.append(x.astype(jnp.bfloat16))
    return jnp.concatenate(parts, axis=0)


def dot_pieces(x, y, dims, count):
    rows = x.shape[0]
    out = lax.dot_general(pieces(x, count), y, (dims, ((), ())), preferred_element_type=jnp.float32)
    total = out[(count - 1) * rows :]
    for k in range(count - 2, -1, -1):
        total = total + out[k * rows : (k + 1) * rows]
    return total


def attend(per_group, per_kv, left, scale, lat, q, uk, uv):
    slots, block_len, width = lat.shape
    rank = width // 2
    heads, head_dim = q.shape
    tokens = slots * block_len
    query = q[...]

    def cols(m, k):
        return m[:, k * head_dim : (k + 1) * head_dim]

    def rows(m, k):
        return m[k * per_kv : (k + 1) * per_kv]

    key_map = uk[...]
    value_map = uv[...]
    absorbed = jnp.concatenate(
        [
            rows(
                lax.dot_general(query, cols(key_map, k), (((1,), (1,)), ((), ())), preferred_element_type=jnp.float32),
                k,
            )
            for k in range(per_group)
        ],
        axis=0,
    )
    key_lat = lat[:, :, :rank].reshape(tokens, rank)
    value_lat = lat[:, :, rank:].reshape(tokens, rank)
    scores = dot_pieces(absorbed, key_lat, ((1,), (1,)), 3) * scale
    live = lax.broadcasted_iota(jnp.int32, (heads, tokens), 1) < left
    scores = jnp.where(live, scores, -1e30)
    largest = jnp.max(scores, axis=1, keepdims=True)
    weights = jnp.where(live, jnp.exp(scores - largest), 0.0)
    total = jnp.sum(weights, axis=1, keepdims=True)
    some = jnp.where(total > 0.0, total, 1.0)
    mixed = dot_pieces(weights, value_lat, ((1,), (0,)), 3) / some
    values = jnp.concatenate(
        [rows(dot_pieces(mixed, cols(value_map, k), ((1,), (0,)), 3), k) for k in range(per_group)], axis=0
    )
    return values, jnp.where(total > 0.0, largest + jnp.log(some), -1e30)


def kernel(
    grps,
    seqs,
    per_seq,
    per_group,
    per_kv,
    dest_hbm,
    len_hbm,
    lat_hbm,
    q_hbm,
    uk_hbm,
    uv_hbm,
    recv_ref,
    att_ref,
    dest_s,
    len_s,
    from_s,
    lat_v,
    q_v,
    uk_v,
    uv_v,
    out_v,
    part_v,
    all_v,
    in_sems,
    send_a,
    recv_near,
    recv_far,
    send_z,
    recv_z,
    send_p,
    recv_p,
    send_c,
    recv_c,
    send_b,
    recv_b,
    send_x,
    send_d,
    plane_sem,
    line_sem,
    all_sem,
    go_sem,
    top_sem,
    mid_sem,
):
    n = grps * seqs
    chips = seqs // CORES
    half = grps // 2
    group = lax.axis_index("grp")
    shard = lax.axis_index("seq")
    me = group * seqs + shard
    spot = shard // CORES
    core = lax.rem(shard, CORES)
    side = group // half
    first_far = (1 - side) * half
    leads = core == CORES - 1
    outer = (group == 0) | (group == grps - 1)
    inner = (group > 0) & (group < grps - 1)
    last = (group == grps - 1) & (spot == chips - 1)
    bits = [lax.rem(spot // 2**b, 2) for b in range(chips.bit_length() - 1)]
    slots, block_len, width = lat_v.shape
    heads, head_dim = q_v.shape
    barrier = pltpu.get_barrier_semaphore()

    def signal(sem, there):
        pl.semaphore_signal(sem, inc=1, device_id=there, device_id_type=MESH)

    def send(src, dst, there, send_sem, recv_sem):
        pltpu.make_async_remote_copy(
            src_ref=src, dst_ref=dst, send_sem=send_sem, recv_sem=recv_sem, device_id=there, device_id_type=MESH
        ).start()

    def wait(some, sem):
        pltpu.make_async_copy(some, some, sem).wait()

    def bits_in(v):
        return sum(bit for b, bit in enumerate(bits) if v >> b & 1)

    def count(of):
        total = 1
        for bit in bits:
            total = total * of(bit)
        return total

    sequence = shard // per_seq
    loads = [
        (dest_hbm, dest_s),
        (lat_hbm.at[0], lat_v),
        (q_hbm.at[sequence, pl.ds(pl.multiple_of(group * heads, heads), heads)], q_v),
        (uk_hbm.at[group], uk_v),
        (uv_hbm.at[group], uv_v),
        (len_hbm, len_s),
    ]
    loads = [pltpu.make_async_copy(src, dst, in_sems.at[i]) for i, (src, dst) in enumerate(loads)]
    for load in loads[:2]:
        load.start()

    with jax.named_scope("sig"):
        for c in range(1, CORES):
            signal(barrier, (group, spot * CORES + lax.rem(core + c, CORES)))
        for v in range(chips):

            @pl.when(bits_in(v) == 0)
            def _():
                @pl.loop(group + (1 if v == 0 else 0), grps)
                def _(g):
                    for c in range(CORES):
                        signal(barrier, (g, (spot + v) * CORES + c))

    for load in loads[2:]:
        load.start()
    with jax.named_scope("w_bar"):
        pl.semaphore_wait(barrier, ((group + 1) * count(lambda bit: 1 + bit) - 1) * CORES + CORES - 1)

    with jax.named_scope("sig2"):
        for v in range(1, chips):

            @pl.when(bits_in(v) == bin(v).count("1"))
            def _():
                signal(plane_sem, (group, (spot - v) * CORES + core))

        @pl.when(group == half)
        def _():
            @pl.loop(0, half)
            def _(g):
                signal(line_sem, (g, shard))

        @pl.when(group == grps - 1)
        def _():
            @pl.loop(0, grps - 1)
            def _(g):
                signal(top_sem, (g, shard))

        @pl.when((group == half) & (spot == chips - 1))
        def _():
            @pl.loop(0, half * chips)
            def _(k):
                signal(mid_sem, (k // chips, lax.rem(k, chips) * CORES + core))

        @pl.when(last)
        def _():
            @pl.loop(0, grps * chips - 1)
            def _(k):
                signal(all_sem, (k // chips, lax.rem(k, chips) * CORES + core))

    with jax.named_scope("w_dest"):
        loads[0].wait()
    lanes = pl.cdiv(n, 128) * 128
    lane = lax.broadcasted_iota(jnp.int32, (1, lanes), 1)

    def place(i, held):
        return jnp.where(lane == dest_s[shard * slots + i], i, held)

    unroll = min(slots, 32)
    source = lax.fori_loop(0, slots, place, jnp.zeros((1, lanes), jnp.int32), unroll=unroll)

    def find(d, _):
        from_s[d] = jnp.sum(jnp.where(lane == d, source, 0))
        return 0

    lax.fori_loop(0, n, find, 0, unroll=unroll)
    with jax.named_scope("w_lat"):
        loads[1].wait()

    def pick(d, _):
        out_v[d] = lat_v[from_s[d]]
        return 0

    with jax.named_scope("pick"):
        lax.fori_loop(0, n, pick, 0, unroll=unroll)
        recv_ref[me] = out_v[me]

    def block(to_group, to_shard, recv_sem):
        send(out_v.at[to_group * seqs + to_shard], recv_ref.at[me], (to_group, to_shard), send_a, recv_sem)

    def turn(table, k):
        if table is None:
            return lax.rem(spot + k, chips)
        return sum(
            row[k] * math.prod(bit if a >> b & 1 else 1 - bit for b, bit in enumerate(bits))
            for a, row in enumerate(table)
            if row[k]
        )

    if chips == 4:
        upper_turns = ((0, 1, 2, 3), (0, 1, 3, 2), (0, 2, 1, 3), (1, 0, 2, 3))
        lower_turns = ((0, 1, 2, 3), (1, 0, 3, 2), (2, 3, 0, 1), (3, 0, 1, 2))
    else:
        upper_turns = lower_turns = None
    ahead_own = (spot == 0) & (core < CORES - 1)
    ahead = (spot > 0) & (core < CORES - 1) & (chips == 4)

    def far_blocks(turns, j, first, end):
        for k in range(first, end):
            to_spot = turn(turns, k)
            for c in range(CORES):
                block(first_far + j, to_spot * CORES + lax.rem(core + c, CORES), recv_far)

    def near_blocks(lowest, highest):
        @pl.loop(lowest, highest)
        def _(g):
            @pl.loop(0, seqs)
            def _(k):
                block(g, lax.rem(shard + k, seqs), recv_near)

    @pl.when(side == 1)
    def _():
        far_blocks(upper_turns, 0, 0, 1)

        @pl.when(ahead)
        def _():
            far_blocks(upper_turns, 0, 1, 2)

        @pl.when(ahead_own)
        def _():
            for j in range(1, half):
                far_blocks(lower_turns, j, 0, 1)

    for load in loads[2:]:
        load.wait()
    with jax.named_scope("attend"):
        left = len_s[sequence] - (shard - sequence * per_seq) * (slots * block_len)
        values, size = attend(per_group, per_kv, left, 1.0 / float(head_dim) ** 0.5, lat_v, q_v, uk_v, uv_v)
        part_v[0:heads, :] = values
        if per_seq > 1:
            part_v[heads : 2 * heads, :] = jnp.broadcast_to(size, (heads, head_dim))

    @pl.loop(side * half, group)
    def _(g):
        send(part_v, all_v.at[spot, group, core], (g, spot * CORES + CORES - 1), send_d, recv_z.at[group])

    @pl.when(core < CORES - 1)
    def _():
        send(part_v, all_v.at[spot, group, core], (group, spot * CORES + CORES - 1), send_c, recv_c)

    @pl.when(leads)
    def _():
        all_v[spot, group, core] = part_v[...]

    @pl.when(side == 0)
    def _():
        with jax.named_scope("w_line"):
            pl.semaphore_wait(line_sem, 1)
        far_blocks(lower_turns, 0, 0, 1)

    with jax.named_scope("w_plane"):

        @pl.when(spot < chips - 1)
        def _():
            pl.semaphore_wait(plane_sem, count(lambda bit: 2 - bit) - 1)

    @pl.loop(1, seqs)
    def _(k):
        block(group, lax.rem(shard + k, seqs), recv_near)

    def along_line(g):
        both = all_v.at[spot, group]
        send(both, both, (g, shard), send_z, recv_z.at[group])

    def over_plane(g):
        both = all_v.at[spot, g]
        for k in range(1, chips):
            send(both, both, (group, lax.rem(spot + k, chips) * CORES + core), send_p, recv_p)

    def release():
        @pl.when(leads)
        def _():
            for c in range(CORES - 1):
                signal(go_sem, (group, spot * CORES + c))
            over_plane(group)

        @pl.when(core < CORES - 1)
        def _():
            pl.semaphore_wait(go_sem, 1)

    @pl.when(core < CORES - 1)
    def _():
        near_blocks(side * half, group)

    @pl.when(leads)
    def _():
        with jax.named_scope("w_part"):
            wait(all_v.at[0, 0, pl.ds(0, CORES - 1)], recv_c)

        @pl.when(side == 1)
        def _():
            along_line(0)

        near_blocks(side * half, group)

    def parts_up():
        with jax.named_scope("w_top"):

            @pl.when(group < grps - 1)
            def _():
                pl.semaphore_wait(top_sem, 1)

        @pl.when(leads)
        def _():
            @pl.loop(group + 1, (side + 1) * half)
            def _(g):
                along_line(g)

            @pl.when(side == 0)
            def _():
                along_line(grps - 1)

    def pass_on():
        @pl.when(leads & outer)
        def _():
            for k in range(half):
                g = first_far + k
                with jax.named_scope("w_x"):
                    wait(all_v.at[0, 0], recv_z.at[g])
                crossed = all_v.at[spot, g]
                for i in range(1, half):
                    to_group = side * half + lax.rem(group - side * half + i, half)
                    send(crossed, crossed, (to_group, shard), send_x, recv_z.at[g])
                over_plane(g)

    @pl.when(side == 1)
    def _():
        release()
        pass_on()

        @pl.when(jnp.logical_not(ahead))
        def _():
            far_blocks(upper_turns, 0, 1, 2)

        far_blocks(upper_turns, 0, 2, chips)
        for j in range(1, half):
            far_blocks(lower_turns, j, 1, chips)

        @pl.when(jnp.logical_not(ahead_own))
        def _():
            for j in range(1, half):
                far_blocks(lower_turns, j, 0, 1)

    @pl.when(side == 0)
    def _():
        parts_up()
        release()
        with jax.named_scope("w_mid"):
            pl.semaphore_wait(mid_sem, 1)
        near_blocks(group + 1, half)
        pass_on()
        far_blocks(lower_turns, 0, 1, chips)

    with jax.named_scope("w_all"):

        @pl.when(jnp.logical_not(last))
        def _():
            pl.semaphore_wait(all_sem, 1)

    @pl.when(side == 0)
    def _():
        for j in range(1, half):
            far_blocks(lower_turns, j, 1, chips)
        for j in range(1, half):
            far_blocks(lower_turns, j, 0, 1)

    @pl.when(side == 1)
    def _():
        parts_up()
        near_blocks(group + 1, grps)


    @pl.when(leads)
    def _():
        for k in range(1, grps):
            for g in (group - k, group + k):

                @pl.when((g >= 0) & (g < grps) & (inner | ((g >= side * half) & (g < (side + 1) * half))))
                def _():
                    with jax.named_scope("w_z"):
                        wait(all_v.at[0, 0], recv_z.at[g])
                    over_plane(g)

        with jax.named_scope("w_p"):
            wait(all_v.at[pl.ds(0, chips - 1)], recv_p)
        for c in range(CORES - 1):
            send(all_v, all_v, (group, spot * CORES + c), send_b, recv_b)

    @pl.when(core < CORES - 1)
    def _():
        with jax.named_scope("w_c"):
            wait(all_v, recv_b)

    batch = att_ref.shape[0]
    with jax.named_scope("att"):
        for g in range(grps):
            if per_seq == 1:
                held = all_v[:, g].reshape(batch, heads, head_dim)
            else:
                part = all_v[:, g].reshape(batch, per_seq, 2 * heads, head_dim)
                sizes = part[:, :, heads:]
                share = jnp.exp(sizes - jnp.max(sizes, axis=1, keepdims=True))
                held = jnp.sum(part[:, :, :heads] * share, axis=1) / jnp.sum(share, axis=1)
            held = jnp.swapaxes(held, 0, 1)
            for h in range(heads):
                at = (g * heads + h) * head_dim
                att_ref[:, at : at + head_dim] = held[h]

    with jax.named_scope("w_send"):
        wait(recv_ref.at[pl.ds(0, n - 1)], send_a)

    @pl.when(leads)
    def _():
        @pl.loop(0, half - (group - side * half))
        def _(_):
            wait(all_v.at[0, 0], send_z)


        @pl.when(outer)
        def _():
            for _ in range(half - 1):
                wait(all_v.at[0, pl.ds(0, half)], send_x)

        wait(all_v.at[pl.ds(0, chips - 1)], send_p)
        for c in range(CORES - 1):
            wait(all_v, send_b)

    @pl.when(core < CORES - 1)
    def _():
        wait(part_v, send_c)

    @pl.loop(side * half, group)
    def _(_):
        wait(part_v, send_d)

    with jax.named_scope("w_near"):
        wait(recv_ref.at[pl.ds(0, n // 2 - 1)], recv_near)
    with jax.named_scope("w_far"):
        wait(recv_ref.at[pl.ds(0, n // 2)], recv_far)


def write_kernel(recv_ref, att_ref, latent_out, attended_out, sems):
    copies = [
        pltpu.make_async_copy(recv_ref, latent_out, sems.at[0]),
        pltpu.make_async_copy(att_ref, attended_out, sems.at[1]),
    ]
    for copy in copies:
        copy.start()
    for copy in copies:
        copy.wait()


def body(grps, seqs, latent, up_key, up_value, queries, lengths, block_dest):
    groups, rank, maps = up_key.shape
    slots, block_len, width = latent.shape[1:]
    batch, q_heads, head_dim = queries.shape
    per_group = maps // head_dim
    heads = q_heads // groups
    per_kv = heads // per_group
    n = grps * seqs
    blk_seq = block_dest.shape[0] // batch
    per_seq = blk_seq // slots
    assert per_seq * slots == blk_seq and n == slots and groups == grps
    assert grps % 2 == 0 and seqs % CORES == 0 and seqs // CORES & (seqs // CORES - 1) == 0
    part_rows = heads if per_seq == 1 else 2 * heads
    anywhere = pl.BlockSpec(memory_space=pl.ANY)
    vmem = pl.BlockSpec(memory_space=pltpu.VMEM)
    dma = pltpu.SemaphoreType.DMA
    received, attended = pl.pallas_call(
        functools.partial(kernel, grps, seqs, per_seq, per_group, per_kv),
        out_shape=(
            pltpu.VMEM((n, block_len, width), latent.dtype),
            pltpu.VMEM((batch, q_heads * head_dim), jnp.float32),
        ),
        in_specs=[anywhere] * 6,
        out_specs=(vmem, vmem),
        scratch_shapes=[
            pltpu.SMEM(block_dest.shape, jnp.int32),
            pltpu.SMEM(lengths.shape, jnp.int32),
            pltpu.SMEM((n,), jnp.int32),
            pltpu.VMEM((slots, block_len, width), latent.dtype),
            pltpu.VMEM((heads, head_dim), queries.dtype),
            pltpu.VMEM((rank, maps), up_key.dtype),
            pltpu.VMEM((rank, maps), up_value.dtype),
            pltpu.VMEM((n, block_len, width), latent.dtype),
            pltpu.VMEM((part_rows, head_dim), jnp.float32),
            pltpu.VMEM((seqs // CORES, grps, CORES, part_rows, head_dim), jnp.float32),
            dma((6,)),
        ]
        + [dma] * 4
        + [dma((grps,))]
        + [dma] * 8
        + [pltpu.SemaphoreType.REGULAR] * 6,
        compiler_params=pltpu.CompilerParams(collective_id=0, has_side_effects=True),
        name="exchange",
    )(block_dest, lengths, latent, queries, up_key, up_value)
    decode_latent, attended = pl.pallas_call(
        write_kernel,
        out_shape=(
            jax.ShapeDtypeStruct(received.shape, received.dtype),
            jax.ShapeDtypeStruct(attended.shape, attended.dtype),
        ),
        in_specs=[anywhere] * 2,
        out_specs=(anywhere, anywhere),
        scratch_shapes=[dma((2,))],
        name="write_out",
    )(pltpu.with_memory_space_constraint(received, pltpu.VMEM), pltpu.with_memory_space_constraint(attended, pltpu.VMEM))
    return (decode_latent.reshape(1, groups, seqs, block_len, width), attended)


def solution(mesh):
    return jax.shard_map(
        functools.partial(body, mesh.shape["grp"], mesh.shape["seq"]),
        mesh=mesh,
        in_specs=(P("grp", "seq", None, None), P(), P(), P(), P(), P()),
        out_specs=(P(("grp", "seq"), None, None, None, None), P()),
        check_vma=False,
    )
```

```python
import functools
import math

import jax
import jax.numpy as jnp
from jax import lax
from jax.experimental import pallas as pl
from jax.experimental.pallas import tpu as pltpu
from jax.sharding import PartitionSpec as P

MESH = pl.DeviceIdType.MESH
CORES = 2


def pieces(x, count):
    parts = []
    for _ in range(count - 1):
        part = x.astype(jnp.bfloat16)
        parts.append(part)
        x = x - part.astype(jnp.float32)
    parts.append(x.astype(jnp.bfloat16))
    return jnp.concatenate(parts, axis=0)


def dot_pieces(x, y, dims, count):
    rows = x.shape[0]
    out = lax.dot_general(pieces(x, count), y, (dims, ((), ())), preferred_element_type=jnp.float32)
    total = out[(count - 1) * rows :]
    for k in range(count - 2, -1, -1):
        total = total + out[k * rows : (k + 1) * rows]
    return total


def attend(per_group, per_kv, left, scale, lat, q, uk, uv):
    slots, block_len, width = lat.shape
    rank = width // 2
    heads, head_dim = q.shape
    tokens = slots * block_len
    query = q[...]

    def cols(m, k):
        return m[:, k * head_dim : (k + 1) * head_dim]

    def rows(m, k):
        return m[k * per_kv : (k + 1) * per_kv]

    key_map = uk[...]
    value_map = uv[...]
    absorbed = jnp.concatenate(
        [
            rows(
                lax.dot_general(query, cols(key_map, k), (((1,), (1,)), ((), ())), preferred_element_type=jnp.float32),
                k,
            )
            for k in range(per_group)
        ],
        axis=0,
    )
    key_lat = lat[:, :, :rank].reshape(tokens, rank)
    value_lat = lat[:, :, rank:].reshape(tokens, rank)
    scores = dot_pieces(absorbed, key_lat, ((1,), (1,)), 3) * scale
    live = lax.broadcasted_iota(jnp.int32, (heads, tokens), 1) < left
    scores = jnp.where(live, scores, -1e30)
    largest = jnp.max(scores, axis=1, keepdims=True)
    weights = jnp.where(live, jnp.exp(scores - largest), 0.0)
    total = jnp.sum(weights, axis=1, keepdims=True)
    some = jnp.where(total > 0.0, total, 1.0)
    mixed = dot_pieces(weights, value_lat, ((1,), (0,)), 3) / some
    values = jnp.concatenate(
        [rows(dot_pieces(mixed, cols(value_map, k), ((1,), (0,)), 3), k) for k in range(per_group)], axis=0
    )
    return values, jnp.where(total > 0.0, largest + jnp.log(some), -1e30)


def kernel(
    grps,
    seqs,
    per_seq,
    per_group,
    per_kv,
    dest_hbm,
    len_hbm,
    lat_hbm,
    q_hbm,
    uk_hbm,
    uv_hbm,
    recv_ref,
    att_ref,
    dest_s,
    len_s,
    from_s,
    lat_v,
    q_v,
    uk_v,
    uv_v,
    out_v,
    relay_v,
    part_v,
    all_v,
    in_sems,
    send_a,
    recv_near,
    recv_far,
    send_z,
    recv_z,
    send_p,
    recv_p,
    send_c,
    recv_c,
    send_b,
    recv_b,
    send_x,
    send_d,
    send_r,
    recv_r,
    plane_sem,
    line_sem,
    all_sem,
    go_sem,
    top_sem,
    mid_sem,
):
    n = grps * seqs
    chips = seqs // CORES
    half = grps // 2
    group = lax.axis_index("grp")
    shard = lax.axis_index("seq")
    me = group * seqs + shard
    spot = shard // CORES
    core = lax.rem(shard, CORES)
    side = group // half
    first_far = (1 - side) * half
    leads = core == CORES - 1
    outer = (group == 0) | (group == grps - 1)
    inner = (group > 0) & (group < grps - 1)
    last = (group == grps - 1) & (spot == chips - 1)
    bits = [lax.rem(spot // 2**b, 2) for b in range(chips.bit_length() - 1)]
    slots, block_len, width = lat_v.shape
    heads, head_dim = q_v.shape
    barrier = pltpu.get_barrier_semaphore()

    def signal(sem, there):
        pl.semaphore_signal(sem, inc=1, device_id=there, device_id_type=MESH)

    def send(src, dst, there, send_sem, recv_sem):
        pltpu.make_async_remote_copy(
            src_ref=src, dst_ref=dst, send_sem=send_sem, recv_sem=recv_sem, device_id=there, device_id_type=MESH
        ).start()

    def wait(some, sem):
        pltpu.make_async_copy(some, some, sem).wait()

    def bits_in(v):
        return sum(bit for b, bit in enumerate(bits) if v >> b & 1)

    def count(of):
        total = 1
        for bit in bits:
            total = total * of(bit)
        return total

    sequence = shard // per_seq
    loads = [
        (dest_hbm, dest_s),
        (lat_hbm.at[0], lat_v),
        (q_hbm.at[sequence, pl.ds(pl.multiple_of(group * heads, heads), heads)], q_v),
        (uk_hbm.at[group], uk_v),
        (uv_hbm.at[group], uv_v),
        (len_hbm, len_s),
    ]
    loads = [pltpu.make_async_copy(src, dst, in_sems.at[i]) for i, (src, dst) in enumerate(loads)]
    for load in loads[:2]:
        load.start()

    with jax.named_scope("sig"):
        for c in range(1, CORES):
            signal(barrier, (group, spot * CORES + lax.rem(core + c, CORES)))
        for v in range(chips):

            @pl.when(bits_in(v) == 0)
            def _():
                @pl.loop(group + (1 if v == 0 else 0), grps)
                def _(g):
                    for c in range(CORES):
                        signal(barrier, (g, (spot + v) * CORES + c))

    for load in loads[2:]:
        load.start()
    with jax.named_scope("w_bar"):
        pl.semaphore_wait(barrier, ((group + 1) * count(lambda bit: 1 + bit) - 1) * CORES + CORES - 1)

    with jax.named_scope("sig2"):
        for v in range(1, chips):

            @pl.when(bits_in(v) == bin(v).count("1"))
            def _():
                signal(plane_sem, (group, (spot - v) * CORES + core))

        @pl.when(group == half)
        def _():
            @pl.loop(0, half)
            def _(g):
                signal(line_sem, (g, shard))

        @pl.when(group == grps - 1)
        def _():
            @pl.loop(0, grps - 1)
            def _(g):
                signal(top_sem, (g, shard))

        @pl.when((group == half) & (spot == chips - 1))
        def _():
            @pl.loop(0, half * chips)
            def _(k):
                signal(mid_sem, (k // chips, lax.rem(k, chips) * CORES + core))

        @pl.when(last)
        def _():
            @pl.loop(0, grps * chips - 1)
            def _(k):
                signal(all_sem, (k // chips, lax.rem(k, chips) * CORES + core))

    with jax.named_scope("w_dest"):
        loads[0].wait()
    lanes = pl.cdiv(n, 128) * 128
    lane = lax.broadcasted_iota(jnp.int32, (1, lanes), 1)

    def place(i, held):
        return jnp.where(lane == dest_s[shard * slots + i], i, held)

    unroll = min(slots, 32)
    source = lax.fori_loop(0, slots, place, jnp.zeros((1, lanes), jnp.int32), unroll=unroll)

    def find(d, _):
        from_s[d] = jnp.sum(jnp.where(lane == d, source, 0))
        return 0

    lax.fori_loop(0, n, find, 0, unroll=unroll)
    with jax.named_scope("w_lat"):
        loads[1].wait()

    def pick(d, _):
        out_v[d] = lat_v[from_s[d]]
        return 0

    with jax.named_scope("pick"):
        lax.fori_loop(0, n, pick, 0, unroll=unroll)
        recv_ref[me] = out_v[me]

    def block(to_group, to_shard, recv_sem):
        send(out_v.at[to_group * seqs + to_shard], recv_ref.at[me], (to_group, to_shard), send_a, recv_sem)

    def turn(table, k):
        if table is None:
            return lax.rem(spot + k, chips)
        return sum(
            row[k] * math.prod(bit if a >> b & 1 else 1 - bit for b, bit in enumerate(bits))
            for a, row in enumerate(table)
            if row[k]
        )

    if chips == 4:
        upper_turns = ((0, 1, 2, 3), (0, 1, 3, 2), (0, 2, 1, 3), (1, 0, 2, 3))
        lower_turns = ((0, 3, 1, 2), (1, 2, 0, 3), (2, 1, 0, 3), (3, 0, 1, 2))
    else:
        upper_turns = lower_turns = None
    ahead_own = (spot == 0) & (core < CORES - 1)
    ahead = (spot > 0) & (core < CORES - 1) & (chips == 4)

    def far_blocks(turns, j, first, end):
        for k in range(first, end):
            to_spot = turn(turns, k)
            for c in range(CORES):
                block(first_far + j, to_spot * CORES + lax.rem(core + c, CORES), recv_far)

    detour = lower_turns is not None and half > 1
    turns_off = (group == half - 1 + side) & (spot == chips - 1) & (core == side)
    relays = (group == half - 1 + side) & (spot == 0) & (core == side)
    off_spot = lower_turns[-1][-1] if detour else 0
    off_group = first_far + half - 1

    def later_blocks():
        for j in range(1, half):
            far_blocks(lower_turns, j, 1, chips - 1)
            if not detour or j < half - 1:
                far_blocks(lower_turns, j, chips - 1, chips)
        if detour:

            @pl.when(jnp.logical_not(turns_off))
            def _():
                far_blocks(lower_turns, half - 1, chips - 1, chips)

            @pl.when(relays)
            def _():
                wait(relay_v, recv_r)
                source_row = group * seqs + (chips - 1) * CORES + core
                for c in range(CORES):
                    there = (off_group, off_spot * CORES + c)
                    send(relay_v.at[c], recv_ref.at[source_row], there, send_r, recv_far)

    def near_blocks(lowest, highest):
        @pl.loop(lowest, highest)
        def _(g):
            @pl.loop(0, seqs)
            def _(k):
                block(g, lax.rem(shard + k, seqs), recv_near)

    @pl.when(side == 1)
    def _():
        far_blocks(upper_turns, 0, 0, 1)

        @pl.when(ahead)
        def _():
            far_blocks(upper_turns, 0, 1, 2)

        @pl.when(ahead_own)
        def _():
            for j in range(1, half):
                far_blocks(lower_turns, j, 0, 1)

    for load in loads[2:]:
        load.wait()
    with jax.named_scope("attend"):
        left = len_s[sequence] - (shard - sequence * per_seq) * (slots * block_len)
        values, size = attend(per_group, per_kv, left, 1.0 / float(head_dim) ** 0.5, lat_v, q_v, uk_v, uv_v)
        part_v[0:heads, :] = values
        if per_seq > 1:
            part_v[heads : 2 * heads, :] = jnp.broadcast_to(size, (heads, head_dim))

    @pl.loop(side * half, group)
    def _(g):
        send(part_v, all_v.at[spot, group, core], (g, spot * CORES + CORES - 1), send_d, recv_z.at[group])

    @pl.when(core < CORES - 1)
    def _():
        send(part_v, all_v.at[spot, group, core], (group, spot * CORES + CORES - 1), send_c, recv_c)

    @pl.when(leads)
    def _():
        all_v[spot, group, core] = part_v[...]

    @pl.when(side == 0)
    def _():
        with jax.named_scope("w_line"):
            pl.semaphore_wait(line_sem, 1)
        far_blocks(lower_turns, 0, 0, 1)

    with jax.named_scope("w_plane"):

        @pl.when(spot < chips - 1)
        def _():
            pl.semaphore_wait(plane_sem, count(lambda bit: 2 - bit) - 1)

    if detour:

        @pl.when(turns_off)
        def _():
            for c in range(CORES):
                held = out_v.at[off_group * seqs + off_spot * CORES + c]
                send(held, relay_v.at[c], (group, core), send_a, recv_r)

    @pl.loop(1, seqs)
    def _(k):
        block(group, lax.rem(shard + k, seqs), recv_near)

    def along_line(g):
        both = all_v.at[spot, group]
        send(both, both, (g, shard), send_z, recv_z.at[group])

    def over_plane(g):
        both = all_v.at[spot, g]
        for k in range(1, chips):
            send(both, both, (group, lax.rem(spot + k, chips) * CORES + core), send_p, recv_p)

    def release():
        @pl.when(leads)
        def _():
            for c in range(CORES - 1):
                signal(go_sem, (group, spot * CORES + c))
            over_plane(group)

        @pl.when(core < CORES - 1)
        def _():
            pl.semaphore_wait(go_sem, 1)

    @pl.when(core < CORES - 1)
    def _():
        near_blocks(side * half, group)

    @pl.when(leads)
    def _():
        with jax.named_scope("w_part"):
            wait(all_v.at[0, 0, pl.ds(0, CORES - 1)], recv_c)

        @pl.when(side == 1)
        def _():
            along_line(0)

        near_blocks(side * half, group)

    def parts_up():
        with jax.named_scope("w_top"):

            @pl.when(group < grps - 1)
            def _():
                pl.semaphore_wait(top_sem, 1)

        @pl.when(leads)
        def _():
            @pl.loop(group + 1, (side + 1) * half)
            def _(g):
                along_line(g)

            @pl.when(side == 0)
            def _():
                along_line(grps - 1)

    def pass_on():
        @pl.when(leads & outer)
        def _():
            for k in range(half):
                g = first_far + k
                with jax.named_scope("w_x"):
                    wait(all_v.at[0, 0], recv_z.at[g])
                crossed = all_v.at[spot, g]
                for i in range(1, half):
                    to_group = side * half + lax.rem(group - side * half + i, half)
                    send(crossed, crossed, (to_group, shard), send_x, recv_z.at[g])
                over_plane(g)

    @pl.when(side == 1)
    def _():
        release()
        pass_on()

        @pl.when(jnp.logical_not(ahead))
        def _():
            far_blocks(upper_turns, 0, 1, 2)

        far_blocks(upper_turns, 0, 2, chips)
        later_blocks()

        @pl.when(jnp.logical_not(ahead_own))
        def _():
            for j in range(1, half):
                far_blocks(lower_turns, j, 0, 1)

    @pl.when(side == 0)
    def _():
        parts_up()
        release()
        with jax.named_scope("w_mid"):
            pl.semaphore_wait(mid_sem, 1)
        near_blocks(group + 1, half)
        pass_on()
        far_blocks(lower_turns, 0, 1, chips)

    with jax.named_scope("w_all"):

        @pl.when(jnp.logical_not(last))
        def _():
            pl.semaphore_wait(all_sem, 1)

    @pl.when(side == 0)
    def _():
        later_blocks()
        for j in range(1, half):
            far_blocks(lower_turns, j, 0, 1)

    @pl.when(side == 1)
    def _():
        parts_up()
        near_blocks(group + 1, grps)


    @pl.when(leads)
    def _():
        for k in range(1, grps):
            for g in (group - k, group + k):

                @pl.when((g >= 0) & (g < grps) & (inner | ((g >= side * half) & (g < (side + 1) * half))))
                def _():
                    with jax.named_scope("w_z"):
                        wait(all_v.at[0, 0], recv_z.at[g])
                    over_plane(g)

        with jax.named_scope("w_p"):
            wait(all_v.at[pl.ds(0, chips - 1)], recv_p)
        for c in range(CORES - 1):
            send(all_v, all_v, (group, spot * CORES + c), send_b, recv_b)

    @pl.when(core < CORES - 1)
    def _():
        with jax.named_scope("w_c"):
            wait(all_v, recv_b)

    batch = att_ref.shape[0]
    with jax.named_scope("att"):
        for g in range(grps):
            if per_seq == 1:
                held = all_v[:, g].reshape(batch, heads, head_dim)
            else:
                part = all_v[:, g].reshape(batch, per_seq, 2 * heads, head_dim)
                sizes = part[:, :, heads:]
                share = jnp.exp(sizes - jnp.max(sizes, axis=1, keepdims=True))
                held = jnp.sum(part[:, :, :heads] * share, axis=1) / jnp.sum(share, axis=1)
            held = jnp.swapaxes(held, 0, 1)
            for h in range(heads):
                at = (g * heads + h) * head_dim
                att_ref[:, at : at + head_dim] = held[h]

    with jax.named_scope("w_send"):
        wait(recv_ref.at[pl.ds(0, n - 1)], send_a)

    @pl.when(leads)
    def _():
        @pl.loop(0, half - (group - side * half))
        def _(_):
            wait(all_v.at[0, 0], send_z)


        @pl.when(outer)
        def _():
            for _ in range(half - 1):
                wait(all_v.at[0, pl.ds(0, half)], send_x)

        wait(all_v.at[pl.ds(0, chips - 1)], send_p)
        for c in range(CORES - 1):
            wait(all_v, send_b)

    if detour:

        @pl.when(relays)
        def _():
            wait(relay_v, send_r)

    @pl.when(core < CORES - 1)
    def _():
        wait(part_v, send_c)

    @pl.loop(side * half, group)
    def _(_):
        wait(part_v, send_d)

    with jax.named_scope("w_near"):
        wait(recv_ref.at[pl.ds(0, n // 2 - 1)], recv_near)
    with jax.named_scope("w_far"):
        wait(recv_ref.at[pl.ds(0, n // 2)], recv_far)


def write_kernel(recv_ref, att_ref, latent_out, attended_out, sems):
    copies = [
        pltpu.make_async_copy(recv_ref, latent_out, sems.at[0]),
        pltpu.make_async_copy(att_ref, attended_out, sems.at[1]),
    ]
    for copy in copies:
        copy.start()
    for copy in copies:
        copy.wait()


def body(grps, seqs, latent, up_key, up_value, queries, lengths, block_dest):
    groups, rank, maps = up_key.shape
    slots, block_len, width = latent.shape[1:]
    batch, q_heads, head_dim = queries.shape
    per_group = maps // head_dim
    heads = q_heads // groups
    per_kv = heads // per_group
    n = grps * seqs
    blk_seq = block_dest.shape[0] // batch
    per_seq = blk_seq // slots
    assert per_seq * slots == blk_seq and n == slots and groups == grps
    assert grps % 2 == 0 and seqs % CORES == 0 and seqs // CORES & (seqs // CORES - 1) == 0
    part_rows = heads if per_seq == 1 else 2 * heads
    anywhere = pl.BlockSpec(memory_space=pl.ANY)
    vmem = pl.BlockSpec(memory_space=pltpu.VMEM)
    dma = pltpu.SemaphoreType.DMA
    received, attended = pl.pallas_call(
        functools.partial(kernel, grps, seqs, per_seq, per_group, per_kv),
        out_shape=(
            pltpu.VMEM((n, block_len, width), latent.dtype),
            pltpu.VMEM((batch, q_heads * head_dim), jnp.float32),
        ),
        in_specs=[anywhere] * 6,
        out_specs=(vmem, vmem),
        scratch_shapes=[
            pltpu.SMEM(block_dest.shape, jnp.int32),
            pltpu.SMEM(lengths.shape, jnp.int32),
            pltpu.SMEM((n,), jnp.int32),
            pltpu.VMEM((slots, block_len, width), latent.dtype),
            pltpu.VMEM((heads, head_dim), queries.dtype),
            pltpu.VMEM((rank, maps), up_key.dtype),
            pltpu.VMEM((rank, maps), up_value.dtype),
            pltpu.VMEM((n, block_len, width), latent.dtype),
            pltpu.VMEM((CORES, block_len, width), latent.dtype),
            pltpu.VMEM((part_rows, head_dim), jnp.float32),
            pltpu.VMEM((seqs // CORES, grps, CORES, part_rows, head_dim), jnp.float32),
            dma((6,)),
        ]
        + [dma] * 4
        + [dma((grps,))]
        + [dma] * 10
        + [pltpu.SemaphoreType.REGULAR] * 6,
        compiler_params=pltpu.CompilerParams(collective_id=0, has_side_effects=True),
        name="exchange",
    )(block_dest, lengths, latent, queries, up_key, up_value)
    decode_latent, attended = pl.pallas_call(
        write_kernel,
        out_shape=(
            jax.ShapeDtypeStruct(received.shape, received.dtype),
            jax.ShapeDtypeStruct(attended.shape, attended.dtype),
        ),
        in_specs=[anywhere] * 2,
        out_specs=(anywhere, anywhere),
        scratch_shapes=[dma((2,))],
        name="write_out",
    )(pltpu.with_memory_space_constraint(received, pltpu.VMEM), pltpu.with_memory_space_constraint(attended, pltpu.VMEM))
    return (decode_latent.reshape(1, groups, seqs, block_len, width), attended)


def solution(mesh):
    return jax.shard_map(
        functools.partial(body, mesh.shape["grp"], mesh.shape["seq"]),
        mesh=mesh,
        in_specs=(P("grp", "seq", None, None), P(), P(), P(), P(), P()),
        out_specs=(P(("grp", "seq"), None, None, None, None), P()),
        check_vma=False,
    )
```

```python
import functools
import math

import jax
import jax.numpy as jnp
from jax import lax
from jax.experimental import pallas as pl
from jax.experimental.pallas import tpu as pltpu
from jax.sharding import PartitionSpec as P

MESH = pl.DeviceIdType.MESH
CORES = 2


def pieces(x, count):
    parts = []
    for _ in range(count - 1):
        part = x.astype(jnp.bfloat16)
        parts.append(part)
        x = x - part.astype(jnp.float32)
    parts.append(x.astype(jnp.bfloat16))
    return jnp.concatenate(parts, axis=0)


def dot_pieces(x, y, dims, count):
    rows = x.shape[0]
    out = lax.dot_general(pieces(x, count), y, (dims, ((), ())), preferred_element_type=jnp.float32)
    total = out[(count - 1) * rows :]
    for k in range(count - 2, -1, -1):
        total = total + out[k * rows : (k + 1) * rows]
    return total


def attend(per_group, per_kv, left, scale, lat, q, uk, uv):
    slots, block_len, width = lat.shape
    rank = width // 2
    heads, head_dim = q.shape
    tokens = slots * block_len
    query = q[...]

    def cols(m, k):
        return m[:, k * head_dim : (k + 1) * head_dim]

    def rows(m, k):
        return m[k * per_kv : (k + 1) * per_kv]

    key_map = uk[...]
    value_map = uv[...]
    absorbed = jnp.concatenate(
        [
            rows(
                lax.dot_general(query, cols(key_map, k), (((1,), (1,)), ((), ())), preferred_element_type=jnp.float32),
                k,
            )
            for k in range(per_group)
        ],
        axis=0,
    )
    key_lat = lat[:, :, :rank].reshape(tokens, rank)
    value_lat = lat[:, :, rank:].reshape(tokens, rank)
    scores = dot_pieces(absorbed, key_lat, ((1,), (1,)), 3) * scale
    live = lax.broadcasted_iota(jnp.int32, (heads, tokens), 1) < left
    scores = jnp.where(live, scores, -1e30)
    largest = jnp.max(scores, axis=1, keepdims=True)
    weights = jnp.where(live, jnp.exp(scores - largest), 0.0)
    total = jnp.sum(weights, axis=1, keepdims=True)
    some = jnp.where(total > 0.0, total, 1.0)
    mixed = dot_pieces(weights, value_lat, ((1,), (0,)), 3) / some
    values = jnp.concatenate(
        [rows(dot_pieces(mixed, cols(value_map, k), ((1,), (0,)), 3), k) for k in range(per_group)], axis=0
    )
    return values, jnp.where(total > 0.0, largest + jnp.log(some), -1e30)


def kernel(
    grps,
    seqs,
    per_seq,
    per_group,
    per_kv,
    dest_hbm,
    len_hbm,
    lat_hbm,
    q_hbm,
    uk_hbm,
    uv_hbm,
    recv_ref,
    att_ref,
    dest_s,
    len_s,
    from_s,
    lat_v,
    q_v,
    uk_v,
    uv_v,
    out_v,
    relay_v,
    part_v,
    all_v,
    in_sems,
    recv_a,
    recv_z,
    recv_p,
    recv_c,
    recv_r,
    plane_sem,
    line_sem,
    all_sem,
    go_sem,
    top_sem,
    mid_sem,
):
    n = grps * seqs
    chips = seqs // CORES
    half = grps // 2
    group = lax.axis_index("grp")
    shard = lax.axis_index("seq")
    me = group * seqs + shard
    spot = shard // CORES
    core = lax.rem(shard, CORES)
    side = group // half
    first_far = (1 - side) * half
    leads = core == CORES - 1
    outer = (group == 0) | (group == grps - 1)
    inner = (group > 0) & (group < grps - 1)
    last = (group == grps - 1) & (spot == chips - 1)
    bits = [lax.rem(spot // 2**b, 2) for b in range(chips.bit_length() - 1)]
    slots, block_len, width = lat_v.shape
    heads, head_dim = q_v.shape
    barrier = pltpu.get_barrier_semaphore()
    sends = in_sems.at[0]

    def signal(sem, there):
        pl.semaphore_signal(sem, inc=1, device_id=there, device_id_type=MESH)

    def send(src, dst, there, send_sem, recv_sem):
        pltpu.make_async_remote_copy(
            src_ref=src, dst_ref=dst, send_sem=send_sem, recv_sem=recv_sem, device_id=there, device_id_type=MESH
        ).start()

    def wait(some, sem):
        pltpu.make_async_copy(some, some, sem).wait()

    def bits_in(v):
        return sum(bit for b, bit in enumerate(bits) if v >> b & 1)

    def count(of):
        total = 1
        for bit in bits:
            total = total * of(bit)
        return total

    sequence = shard // per_seq
    loads = [
        (dest_hbm, dest_s),
        (lat_hbm.at[0], lat_v),
        (q_hbm.at[sequence, pl.ds(pl.multiple_of(group * heads, heads), heads)], q_v),
        (uk_hbm.at[group], uk_v),
        (uv_hbm.at[group], uv_v),
        (len_hbm, len_s),
    ]
    loads = [pltpu.make_async_copy(src, dst, in_sems.at[min(i, 2)]) for i, (src, dst) in enumerate(loads)]
    for load in loads[:2]:
        load.start()

    with jax.named_scope("sig"):
        for c in range(1, CORES):
            signal(barrier, (group, spot * CORES + lax.rem(core + c, CORES)))
        for v in range(chips):

            @pl.when(bits_in(v) == 0)
            def _():
                @pl.loop(group + (1 if v == 0 else 0), grps)
                def _(g):
                    for c in range(CORES):
                        signal(barrier, (g, (spot + v) * CORES + c))

    for load in loads[2:]:
        load.start()
    with jax.named_scope("w_bar"):
        pl.semaphore_wait(barrier, ((group + 1) * count(lambda bit: 1 + bit) - 1) * CORES + CORES - 1)

    with jax.named_scope("sig2"):
        for v in range(1, chips):

            @pl.when(bits_in(v) == bin(v).count("1"))
            def _():
                signal(plane_sem, (group, (spot - v) * CORES + core))

        @pl.when(group == half)
        def _():
            @pl.loop(0, half)
            def _(g):
                signal(line_sem, (g, shard))

        @pl.when(group == grps - 1)
        def _():
            @pl.loop(0, grps - 1)
            def _(g):
                signal(top_sem, (g, shard))

        @pl.when((group == half) & (spot == chips - 1))
        def _():
            @pl.loop(0, half * chips)
            def _(k):
                signal(mid_sem, (k // chips, lax.rem(k, chips) * CORES + core))

        @pl.when(last)
        def _():
            @pl.loop(0, grps * chips - 1)
            def _(k):
                signal(all_sem, (k // chips, lax.rem(k, chips) * CORES + core))

    with jax.named_scope("w_dest"):
        loads[0].wait()
    lanes = pl.cdiv(n, 128) * 128
    lane = lax.broadcasted_iota(jnp.int32, (1, lanes), 1)

    def place(i, held):
        return jnp.where(lane == dest_s[shard * slots + i], i, held)

    unroll = min(slots, 32)
    source = lax.fori_loop(0, slots, place, jnp.zeros((1, lanes), jnp.int32), unroll=unroll)

    def find(d, _):
        from_s[d] = jnp.sum(jnp.where(lane == d, source, 0))
        return 0

    lax.fori_loop(0, n, find, 0, unroll=unroll)
    with jax.named_scope("w_lat"):
        loads[1].wait()

    def pick(d, _):
        out_v[d] = lat_v[from_s[d]]
        return 0

    with jax.named_scope("pick"):
        lax.fori_loop(0, n, pick, 0, unroll=unroll)
        recv_ref[me] = out_v[me]

    def block(to_group, to_shard, recv_sem):
        send(out_v.at[to_group * seqs + to_shard], recv_ref.at[me], (to_group, to_shard), sends, recv_sem)

    def turn(table, k):
        if table is None:
            return lax.rem(spot + k, chips)
        return sum(
            row[k] * math.prod(bit if a >> b & 1 else 1 - bit for b, bit in enumerate(bits))
            for a, row in enumerate(table)
            if row[k]
        )

    if chips == 4:
        upper_turns = ((0, 1, 2, 3), (0, 1, 3, 2), (0, 2, 1, 3), (1, 0, 2, 3))
        lower_turns = ((0, 3, 1, 2), (1, 2, 0, 3), (2, 1, 0, 3), (3, 0, 1, 2))
    else:
        upper_turns = lower_turns = None
    ahead_own = (spot == 0) & (core < CORES - 1)
    ahead = (spot > 0) & (core < CORES - 1) & (chips == 4)

    def far_blocks(turns, j, first, end):
        for k in range(first, end):
            to_spot = turn(turns, k)
            for c in range(CORES):
                block(first_far + j, to_spot * CORES + lax.rem(core + c, CORES), recv_a)

    detour = lower_turns is not None and half > 1
    turns_off = (group == half - 1 + side) & (spot == chips - 1) & (core == side)
    relays = (group == half - 1 + side) & (spot == 0) & (core == side)
    off_spot = lower_turns[-1][-1] if detour else 0
    off_group = first_far + half - 1

    def later_blocks():
        for j in range(1, half):
            far_blocks(lower_turns, j, 1, chips - 1)
            if not detour or j < half - 1:
                far_blocks(lower_turns, j, chips - 1, chips)
        if detour:

            @pl.when(jnp.logical_not(turns_off))
            def _():
                far_blocks(lower_turns, half - 1, chips - 1, chips)

            @pl.when(relays)
            def _():
                wait(relay_v, recv_r)
                source_row = group * seqs + (chips - 1) * CORES + core
                for c in range(CORES):
                    there = (off_group, off_spot * CORES + c)
                    send(relay_v.at[c], recv_ref.at[source_row], there, sends, recv_a)

    def near_blocks(lowest, highest):
        @pl.loop(lowest, highest)
        def _(g):
            @pl.loop(0, seqs)
            def _(k):
                block(g, lax.rem(shard + k, seqs), recv_a)

    @pl.when(side == 1)
    def _():
        far_blocks(upper_turns, 0, 0, 1)

        @pl.when(ahead)
        def _():
            far_blocks(upper_turns, 0, 1, 2)

        @pl.when(ahead_own)
        def _():
            for j in range(1, half):
                far_blocks(lower_turns, j, 0, 1)

    for load in loads[2:]:
        load.wait()
    with jax.named_scope("attend"):
        left = len_s[sequence] - (shard - sequence * per_seq) * (slots * block_len)
        values, size = attend(per_group, per_kv, left, 1.0 / float(head_dim) ** 0.5, lat_v, q_v, uk_v, uv_v)
        part_v[0:heads, :] = values
        if per_seq > 1:
            part_v[heads : 2 * heads, :] = jnp.broadcast_to(size, (heads, head_dim))

    @pl.loop(side * half, group)
    def _(g):
        send(part_v, all_v.at[spot, group, core], (g, spot * CORES + CORES - 1), sends, recv_z.at[group])

    @pl.when(core < CORES - 1)
    def _():
        send(part_v, all_v.at[spot, group, core], (group, spot * CORES + CORES - 1), sends, recv_c)

    @pl.when(leads)
    def _():
        all_v[spot, group, core] = part_v[...]

    @pl.when(side == 0)
    def _():
        with jax.named_scope("w_line"):
            pl.semaphore_wait(line_sem, 1)
        far_blocks(lower_turns, 0, 0, 1)

    with jax.named_scope("w_plane"):

        @pl.when(spot < chips - 1)
        def _():
            pl.semaphore_wait(plane_sem, count(lambda bit: 2 - bit) - 1)

    if detour:

        @pl.when(turns_off)
        def _():
            for c in range(CORES):
                held = out_v.at[off_group * seqs + off_spot * CORES + c]
                send(held, relay_v.at[c], (group, core), sends, recv_r)

    @pl.loop(1, seqs)
    def _(k):
        block(group, lax.rem(shard + k, seqs), recv_a)

    def along_line(g):
        both = all_v.at[spot, group]
        send(both, both, (g, shard), sends, recv_z.at[group])

    def over_plane(g):
        both = all_v.at[spot, g]
        for k in range(1, chips):
            send(both, both, (group, lax.rem(spot + k, chips) * CORES + core), sends, recv_p)

    def release():
        @pl.when(leads)
        def _():
            for c in range(CORES - 1):
                signal(go_sem, (group, spot * CORES + c))
            over_plane(group)

        @pl.when(core < CORES - 1)
        def _():
            pl.semaphore_wait(go_sem, 1)

    @pl.when(core < CORES - 1)
    def _():
        near_blocks(side * half, group)

    @pl.when(leads)
    def _():
        with jax.named_scope("w_part"):
            wait(all_v.at[0, 0, pl.ds(0, CORES - 1)], recv_c)

        @pl.when(side == 1)
        def _():
            along_line(0)

        near_blocks(side * half, group)

    def parts_up():
        with jax.named_scope("w_top"):

            @pl.when(group < grps - 1)
            def _():
                pl.semaphore_wait(top_sem, 1)

        @pl.when(leads)
        def _():
            @pl.loop(group + 1, (side + 1) * half)
            def _(g):
                along_line(g)

            @pl.when(side == 0)
            def _():
                along_line(grps - 1)

    def pass_on():
        @pl.when(leads & outer)
        def _():
            for k in range(half):
                g = first_far + k
                with jax.named_scope("w_x"):
                    wait(all_v.at[0, 0], recv_z.at[g])
                crossed = all_v.at[spot, g]
                for i in range(1, half):
                    to_group = side * half + lax.rem(group - side * half + i, half)
                    send(crossed, crossed, (to_group, shard), sends, recv_z.at[g])
                over_plane(g)

    @pl.when(side == 1)
    def _():
        release()
        pass_on()

        @pl.when(jnp.logical_not(ahead))
        def _():
            far_blocks(upper_turns, 0, 1, 2)

        far_blocks(upper_turns, 0, 2, chips)
        later_blocks()

        @pl.when(jnp.logical_not(ahead_own))
        def _():
            for j in range(1, half):
                far_blocks(lower_turns, j, 0, 1)

    @pl.when(side == 0)
    def _():
        parts_up()
        release()
        with jax.named_scope("w_mid"):
            pl.semaphore_wait(mid_sem, 1)
        near_blocks(group + 1, half)
        pass_on()
        far_blocks(lower_turns, 0, 1, chips)

    with jax.named_scope("w_all"):

        @pl.when(jnp.logical_not(last))
        def _():
            pl.semaphore_wait(all_sem, 1)

    @pl.when(side == 0)
    def _():
        later_blocks()
        for j in range(1, half):
            far_blocks(lower_turns, j, 0, 1)

    @pl.when(side == 1)
    def _():
        parts_up()
        near_blocks(group + 1, grps)


    @pl.when(leads)
    def _():
        for k in range(1, grps):
            for g in (group - k, group + k):

                @pl.when((g >= 0) & (g < grps) & (inner | ((g >= side * half) & (g < (side + 1) * half))))
                def _():
                    with jax.named_scope("w_z"):
                        wait(all_v.at[0, 0], recv_z.at[g])
                    over_plane(g)

        with jax.named_scope("w_p"):
            wait(all_v.at[pl.ds(0, chips - 1)], recv_p)
        for c in range(CORES - 1):
            send(all_v, all_v, (group, spot * CORES + c), sends, recv_c)

    @pl.when(core < CORES - 1)
    def _():
        with jax.named_scope("w_c"):
            wait(all_v, recv_c)

    batch = att_ref.shape[0]
    with jax.named_scope("att"):
        for g in range(grps):
            if per_seq == 1:
                held = all_v[:, g].reshape(batch, heads, head_dim)
            else:
                part = all_v[:, g].reshape(batch, per_seq, 2 * heads, head_dim)
                sizes = part[:, :, heads:]
                share = jnp.exp(sizes - jnp.max(sizes, axis=1, keepdims=True))
                held = jnp.sum(part[:, :, :heads] * share, axis=1) / jnp.sum(share, axis=1)
            held = jnp.swapaxes(held, 0, 1)
            for h in range(heads):
                at = (g * heads + h) * head_dim
                att_ref[:, at : at + head_dim] = held[h]

    with jax.named_scope("w_send"):
        wait(recv_ref.at[pl.ds(0, n - 1)], sends)

    @pl.when(leads)
    def _():
        @pl.loop(0, half - (group - side * half))
        def _(_):
            wait(all_v.at[0, 0], sends)


        @pl.when(outer)
        def _():
            for _ in range(half - 1):
                wait(all_v.at[0, pl.ds(0, half)], sends)

        wait(all_v.at[pl.ds(0, chips - 1)], sends)
        for c in range(CORES - 1):
            wait(all_v, sends)

    if detour:

        @pl.when(relays)
        def _():
            wait(relay_v, sends)

    @pl.when(core < CORES - 1)
    def _():
        wait(part_v, sends)

    @pl.loop(side * half, group)
    def _(_):
        wait(part_v, sends)

    with jax.named_scope("w_far"):
        wait(recv_ref.at[pl.ds(0, n - 1)], recv_a)


def write_kernel(recv_ref, att_ref, latent_out, attended_out, sem):
    copies = [
        pltpu.make_async_copy(recv_ref, latent_out, sem),
        pltpu.make_async_copy(att_ref, attended_out, sem),
    ]
    for copy in copies:
        copy.start()
    for copy in copies:
        copy.wait()


def body(grps, seqs, latent, up_key, up_value, queries, lengths, block_dest):
    groups, rank, maps = up_key.shape
    slots, block_len, width = latent.shape[1:]
    batch, q_heads, head_dim = queries.shape
    per_group = maps // head_dim
    heads = q_heads // groups
    per_kv = heads // per_group
    n = grps * seqs
    blk_seq = block_dest.shape[0] // batch
    per_seq = blk_seq // slots
    assert per_seq * slots == blk_seq and n == slots and groups == grps
    assert grps % 2 == 0 and seqs % CORES == 0 and seqs // CORES & (seqs // CORES - 1) == 0
    part_rows = heads if per_seq == 1 else 2 * heads
    anywhere = pl.BlockSpec(memory_space=pl.ANY)
    vmem = pl.BlockSpec(memory_space=pltpu.VMEM)
    dma = pltpu.SemaphoreType.DMA
    received, attended = pl.pallas_call(
        functools.partial(kernel, grps, seqs, per_seq, per_group, per_kv),
        out_shape=(
            pltpu.VMEM((n, block_len, width), latent.dtype),
            pltpu.VMEM((batch, q_heads * head_dim), jnp.float32),
        ),
        in_specs=[anywhere] * 6,
        out_specs=(vmem, vmem),
        scratch_shapes=[
            pltpu.SMEM(block_dest.shape, jnp.int32),
            pltpu.SMEM(lengths.shape, jnp.int32),
            pltpu.SMEM((n,), jnp.int32),
            pltpu.VMEM((slots, block_len, width), latent.dtype),
            pltpu.VMEM((heads, head_dim), queries.dtype),
            pltpu.VMEM((rank, maps), up_key.dtype),
            pltpu.VMEM((rank, maps), up_value.dtype),
            pltpu.VMEM((n, block_len, width), latent.dtype),
            pltpu.VMEM((CORES, block_len, width), latent.dtype),
            pltpu.VMEM((part_rows, head_dim), jnp.float32),
            pltpu.VMEM((seqs // CORES, grps, CORES, part_rows, head_dim), jnp.float32),
            dma((3,)),
            dma,
            dma((grps,)),
        ]
        + [dma] * 3
        + [pltpu.SemaphoreType.REGULAR] * 6,
        compiler_params=pltpu.CompilerParams(collective_id=0, has_side_effects=True),
        name="exchange",
    )(block_dest, lengths, latent, queries, up_key, up_value)
    decode_latent, attended = pl.pallas_call(
        write_kernel,
        out_shape=(
            jax.ShapeDtypeStruct(received.shape, received.dtype),
            jax.ShapeDtypeStruct(attended.shape, attended.dtype),
        ),
        in_specs=[anywhere] * 2,
        out_specs=(anywhere, anywhere),
        scratch_shapes=[dma],
        name="write_out",
    )(pltpu.with_memory_space_constraint(received, pltpu.VMEM), pltpu.with_memory_space_constraint(attended, pltpu.VMEM))
    return (decode_latent.reshape(1, groups, seqs, block_len, width), attended)


def solution(mesh):
    return jax.shard_map(
        functools.partial(body, mesh.shape["grp"], mesh.shape["seq"]),
        mesh=mesh,
        in_specs=(P("grp", "seq", None, None), P(), P(), P(), P(), P()),
        out_specs=(P(("grp", "seq"), None, None, None, None), P()),
        check_vma=False,
    )
```

```python
import functools
import math

import jax
import jax.numpy as jnp
from jax import lax
from jax.experimental import pallas as pl
from jax.experimental.pallas import tpu as pltpu
from jax.sharding import PartitionSpec as P

MESH = pl.DeviceIdType.MESH
CORES = 2


def pieces(x, count):
    parts = []
    for _ in range(count - 1):
        part = x.astype(jnp.bfloat16)
        parts.append(part)
        x = x - part.astype(jnp.float32)
    parts.append(x.astype(jnp.bfloat16))
    return jnp.concatenate(parts, axis=0)


def dot_pieces(x, y, dims, count):
    rows = x.shape[0]
    out = lax.dot_general(pieces(x, count), y, (dims, ((), ())), preferred_element_type=jnp.float32)
    total = out[(count - 1) * rows :]
    for k in range(count - 2, -1, -1):
        total = total + out[k * rows : (k + 1) * rows]
    return total


def attend(per_group, per_kv, left, scale, lat, q, uk, uv):
    slots, block_len, width = lat.shape
    rank = width // 2
    heads, head_dim = q.shape
    tokens = slots * block_len
    query = q[...]

    def cols(m, k):
        return m[:, k * head_dim : (k + 1) * head_dim]

    def rows(m, k):
        return m[k * per_kv : (k + 1) * per_kv]

    key_map = uk[...]
    value_map = uv[...]
    absorbed = jnp.concatenate(
        [
            rows(
                lax.dot_general(query, cols(key_map, k), (((1,), (1,)), ((), ())), preferred_element_type=jnp.float32),
                k,
            )
            for k in range(per_group)
        ],
        axis=0,
    )
    key_lat = lat[:, :, :rank].reshape(tokens, rank)
    value_lat = lat[:, :, rank:].reshape(tokens, rank)
    scores = dot_pieces(absorbed, key_lat, ((1,), (1,)), 3) * scale
    live = lax.broadcasted_iota(jnp.int32, (heads, tokens), 1) < left
    scores = jnp.where(live, scores, -1e30)
    largest = jnp.max(scores, axis=1, keepdims=True)
    weights = jnp.where(live, jnp.exp(scores - largest), 0.0)
    total = jnp.sum(weights, axis=1, keepdims=True)
    some = jnp.where(total > 0.0, total, 1.0)
    mixed = dot_pieces(weights, value_lat, ((1,), (0,)), 3) / some
    values = jnp.concatenate(
        [rows(dot_pieces(mixed, cols(value_map, k), ((1,), (0,)), 3), k) for k in range(per_group)], axis=0
    )
    return values, jnp.where(total > 0.0, largest + jnp.log(some), -1e30)


def kernel(
    grps,
    seqs,
    per_seq,
    per_group,
    per_kv,
    dest_hbm,
    len_hbm,
    lat_hbm,
    q_hbm,
    uk_hbm,
    uv_hbm,
    recv_ref,
    att_ref,
    dest_s,
    len_s,
    from_s,
    lat_v,
    q_v,
    uk_v,
    uv_v,
    out_v,
    relay_v,
    part_v,
    all_v,
    in_sems,
    recv_a,
    recv_z,
    recv_p,
    recv_c,
    recv_r,
    plane_sem,
    line_sem,
    all_sem,
    go_sem,
    top_sem,
    mid_sem,
):
    n = grps * seqs
    chips = seqs // CORES
    half = grps // 2
    group = lax.axis_index("grp")
    shard = lax.axis_index("seq")
    me = group * seqs + shard
    spot = shard // CORES
    core = lax.rem(shard, CORES)
    side = group // half
    first_far = (1 - side) * half
    leads = core == CORES - 1
    outer = (group == 0) | (group == grps - 1)
    inner = (group > 0) & (group < grps - 1)
    last = (group == grps - 1) & (spot == chips - 1)
    bits = [lax.rem(spot // 2**b, 2) for b in range(chips.bit_length() - 1)]
    slots, block_len, width = lat_v.shape
    heads, head_dim = q_v.shape
    barrier = pltpu.get_barrier_semaphore()
    sends = in_sems.at[0]

    def signal(sem, there):
        pl.semaphore_signal(sem, inc=1, device_id=there, device_id_type=MESH)

    def send(src, dst, there, send_sem, recv_sem):
        pltpu.make_async_remote_copy(
            src_ref=src, dst_ref=dst, send_sem=send_sem, recv_sem=recv_sem, device_id=there, device_id_type=MESH
        ).start()

    def wait(some, sem):
        pltpu.make_async_copy(some, some, sem).wait()

    def bits_in(v):
        return sum(bit for b, bit in enumerate(bits) if v >> b & 1)

    def count(of):
        total = 1
        for bit in bits:
            total = total * of(bit)
        return total

    sequence = shard // per_seq
    loads = [
        (dest_hbm, dest_s),
        (lat_hbm.at[0], lat_v),
        (q_hbm.at[sequence, pl.ds(pl.multiple_of(group * heads, heads), heads)], q_v),
        (uk_hbm.at[group], uk_v),
        (uv_hbm.at[group], uv_v),
        (len_hbm, len_s),
    ]
    loads = [pltpu.make_async_copy(src, dst, in_sems.at[min(i, 2)]) for i, (src, dst) in enumerate(loads)]
    for load in loads[:2]:
        load.start()

    with jax.named_scope("sig"):
        for c in range(1, CORES):
            signal(barrier, (group, spot * CORES + lax.rem(core + c, CORES)))
        for v in range(chips):

            @pl.when(bits_in(v) == 0)
            def _():
                @pl.loop(group + (1 if v == 0 else 0), grps)
                def _(g):
                    for c in range(CORES):
                        signal(barrier, (g, (spot + v) * CORES + c))

    for load in loads[2:]:
        load.start()
    with jax.named_scope("w_bar"):
        pl.semaphore_wait(barrier, ((group + 1) * count(lambda bit: 1 + bit) - 1) * CORES + CORES - 1)

    with jax.named_scope("sig2"):
        for v in range(1, chips):

            @pl.when(bits_in(v) == bin(v).count("1"))
            def _():
                signal(plane_sem, (group, (spot - v) * CORES + core))

        @pl.when(group == half)
        def _():
            @pl.loop(0, half)
            def _(g):
                signal(line_sem, (g, shard))

        @pl.when(group == grps - 1)
        def _():
            @pl.loop(0, grps - 1)
            def _(g):
                signal(top_sem, (g, shard))

        @pl.when((group == half) & (spot == chips - 1))
        def _():
            @pl.loop(0, half * chips)
            def _(k):
                signal(mid_sem, (k // chips, lax.rem(k, chips) * CORES + core))

        @pl.when(last)
        def _():
            @pl.loop(0, grps * chips - 1)
            def _(k):
                signal(all_sem, (k // chips, lax.rem(k, chips) * CORES + core))

    with jax.named_scope("w_dest"):
        loads[0].wait()
    lanes = pl.cdiv(n, 128) * 128
    lane = lax.broadcasted_iota(jnp.int32, (1, lanes), 1)

    def place(i, held):
        return jnp.where(lane == dest_s[shard * slots + i], i, held)

    unroll = min(slots, 32)
    source = lax.fori_loop(0, slots, place, jnp.zeros((1, lanes), jnp.int32), unroll=unroll)

    def find(d, _):
        from_s[d] = jnp.sum(jnp.where(lane == d, source, 0))
        return 0

    lax.fori_loop(0, n, find, 0, unroll=unroll)
    with jax.named_scope("w_lat"):
        loads[1].wait()

    def pick(d, _):
        out_v[d] = lat_v[from_s[d]]
        return 0

    with jax.named_scope("pick"):
        lax.fori_loop(0, n, pick, 0, unroll=unroll)
        recv_ref[me] = out_v[me]

    def block(to_group, to_shard, recv_sem):
        send(out_v.at[to_group * seqs + to_shard], recv_ref.at[me], (to_group, to_shard), sends, recv_sem)

    def turn(table, k):
        if table is None:
            return lax.rem(spot + k, chips)
        return sum(
            row[k] * math.prod(bit if a >> b & 1 else 1 - bit for b, bit in enumerate(bits))
            for a, row in enumerate(table)
            if row[k]
        )

    if chips == 4:
        upper_turns = ((0, 1, 2, 3), (0, 1, 3, 2), (0, 2, 1, 3), (1, 0, 2, 3))
        lower_turns = ((0, 3, 1, 2), (1, 2, 0, 3), (2, 1, 0, 3), (3, 0, 1, 2))
    else:
        upper_turns = lower_turns = None
    ahead_own = (spot == 0) & (core < CORES - 1)
    ahead = (spot > 0) & (chips == 4)

    def far_blocks(turns, j, first, end):
        for k in range(first, end):
            to_spot = turn(turns, k)
            for c in range(CORES):
                block(first_far + j, to_spot * CORES + lax.rem(core + c, CORES), recv_a)

    detour = lower_turns is not None and half > 1
    turns_off = (group == half - 1 + side) & (spot == chips - 1) & (core == side)
    relays = (group == half - 1 + side) & (spot == 0) & (core == side)
    off_spot = lower_turns[-1][-1] if detour else 0
    off_group = first_far + half - 1

    def later_blocks():
        for j in range(1, half):
            far_blocks(lower_turns, j, 1, chips - 1)
            if not detour or j < half - 1:
                far_blocks(lower_turns, j, chips - 1, chips)
        if detour:

            @pl.when(jnp.logical_not(turns_off))
            def _():
                far_blocks(lower_turns, half - 1, chips - 1, chips)

            @pl.when(turns_off)
            def _():
                block(off_group, off_spot * CORES + 0, recv_a)

            @pl.when(relays)
            def _():
                wait(relay_v, recv_r)
                source_row = group * seqs + (chips - 1) * CORES + core
                send(relay_v, recv_ref.at[source_row], (off_group, off_spot * CORES + 1), sends, recv_a)

    def near_blocks(lowest, highest):
        @pl.loop(lowest, highest)
        def _(g):
            @pl.loop(0, seqs)
            def _(k):
                block(g, lax.rem(shard + k, seqs), recv_a)

    @pl.when(side == 1)
    def _():
        far_blocks(upper_turns, 0, 0, 1)

        @pl.when(ahead)
        def _():
            far_blocks(upper_turns, 0, 1, 2)

        @pl.when(ahead_own)
        def _():
            for j in range(1, half):
                far_blocks(lower_turns, j, 0, 1)

    for load in loads[2:]:
        load.wait()
    with jax.named_scope("attend"):
        left = len_s[sequence] - (shard - sequence * per_seq) * (slots * block_len)
        values, size = attend(per_group, per_kv, left, 1.0 / float(head_dim) ** 0.5, lat_v, q_v, uk_v, uv_v)
        part_v[0:heads, :] = values
        if per_seq > 1:
            part_v[heads : 2 * heads, :] = jnp.broadcast_to(size, (heads, head_dim))

    @pl.loop(side * half, group)
    def _(g):
        send(part_v, all_v.at[spot, group, core], (g, spot * CORES + CORES - 1), sends, recv_z.at[group])

    @pl.when(core < CORES - 1)
    def _():
        send(part_v, all_v.at[spot, group, core], (group, spot * CORES + CORES - 1), sends, recv_c)

    @pl.when(leads)
    def _():
        all_v[spot, group, core] = part_v[...]

    @pl.when(side == 0)
    def _():
        with jax.named_scope("w_line"):
            pl.semaphore_wait(line_sem, 1)
        far_blocks(lower_turns, 0, 0, 1)

    with jax.named_scope("w_plane"):

        @pl.when(spot < chips - 1)
        def _():
            pl.semaphore_wait(plane_sem, count(lambda bit: 2 - bit) - 1)

    if detour:

        @pl.when(turns_off)
        def _():
            held = out_v.at[off_group * seqs + off_spot * CORES + 1]
            send(held, relay_v, (group, core), sends, recv_r)

    @pl.loop(1, seqs)
    def _(k):
        block(group, lax.rem(shard + k, seqs), recv_a)

    def along_line(g):
        both = all_v.at[spot, group]
        send(both, both, (g, shard), sends, recv_z.at[group])

    def over_plane(g):
        both = all_v.at[spot, g]
        for k in range(1, chips):
            send(both, both, (group, lax.rem(spot + k, chips) * CORES + core), sends, recv_p)

    def release():
        @pl.when(leads)
        def _():
            for c in range(CORES - 1):
                signal(go_sem, (group, spot * CORES + c))
            over_plane(group)

        @pl.when(core < CORES - 1)
        def _():
            pl.semaphore_wait(go_sem, 1)

    @pl.when(core < CORES - 1)
    def _():
        near_blocks(side * half, group)

    @pl.when(leads)
    def _():
        with jax.named_scope("w_part"):
            wait(all_v.at[0, 0, pl.ds(0, CORES - 1)], recv_c)

        @pl.when(side == 1)
        def _():
            along_line(0)

        near_blocks(side * half, group)

    def parts_up():
        with jax.named_scope("w_top"):

            @pl.when(group < grps - 1)
            def _():
                pl.semaphore_wait(top_sem, 1)

        @pl.when(leads)
        def _():
            @pl.loop(group + 1, (side + 1) * half)
            def _(g):
                along_line(g)

            @pl.when(side == 0)
            def _():
                along_line(grps - 1)

    def pass_on():
        @pl.when(leads & outer)
        def _():
            for k in range(half):
                g = first_far + k
                with jax.named_scope("w_x"):
                    wait(all_v.at[0, 0], recv_z.at[g])
                crossed = all_v.at[spot, g]
                for i in range(1, half):
                    to_group = side * half + lax.rem(group - side * half + i, half)
                    send(crossed, crossed, (to_group, shard), sends, recv_z.at[g])
                over_plane(g)

    @pl.when(side == 1)
    def _():
        release()
        pass_on()

        @pl.when(jnp.logical_not(ahead))
        def _():
            far_blocks(upper_turns, 0, 1, 2)

        far_blocks(upper_turns, 0, 2, chips)
        later_blocks()

        @pl.when(jnp.logical_not(ahead_own))
        def _():
            for j in range(1, half):
                far_blocks(lower_turns, j, 0, 1)

    @pl.when(side == 0)
    def _():
        parts_up()
        release()
        with jax.named_scope("w_mid"):
            pl.semaphore_wait(mid_sem, 1)
        near_blocks(group + 1, half)
        pass_on()
        far_blocks(lower_turns, 0, 1, chips)

    with jax.named_scope("w_all"):

        @pl.when(jnp.logical_not(last))
        def _():
            pl.semaphore_wait(all_sem, 1)

    @pl.when(side == 0)
    def _():
        later_blocks()
        for j in range(1, half):
            far_blocks(lower_turns, j, 0, 1)

    @pl.when(side == 1)
    def _():
        parts_up()
        near_blocks(group + 1, grps)


    @pl.when(leads)
    def _():
        for k in range(1, grps):
            for g in (group - k, group + k):

                @pl.when((g >= 0) & (g < grps) & (inner | ((g >= side * half) & (g < (side + 1) * half))))
                def _():
                    with jax.named_scope("w_z"):
                        wait(all_v.at[0, 0], recv_z.at[g])
                    over_plane(g)

        with jax.named_scope("w_p"):
            wait(all_v.at[pl.ds(0, chips - 1)], recv_p)
        for c in range(CORES - 1):
            send(all_v, all_v, (group, spot * CORES + c), sends, recv_c)

    @pl.when(core < CORES - 1)
    def _():
        with jax.named_scope("w_c"):
            wait(all_v, recv_c)

    batch = att_ref.shape[0]
    with jax.named_scope("att"):
        for g in range(grps):
            if per_seq == 1:
                held = all_v[:, g].reshape(batch, heads, head_dim)
            else:
                part = all_v[:, g].reshape(batch, per_seq, 2 * heads, head_dim)
                sizes = part[:, :, heads:]
                share = jnp.exp(sizes - jnp.max(sizes, axis=1, keepdims=True))
                held = jnp.sum(part[:, :, :heads] * share, axis=1) / jnp.sum(share, axis=1)
            held = jnp.swapaxes(held, 0, 1)
            for h in range(heads):
                at = (g * heads + h) * head_dim
                att_ref[:, at : at + head_dim] = held[h]

    with jax.named_scope("w_send"):
        wait(recv_ref.at[pl.ds(0, n - 1)], sends)

    @pl.when(leads)
    def _():
        @pl.loop(0, half - (group - side * half))
        def _(_):
            wait(all_v.at[0, 0], sends)


        @pl.when(outer)
        def _():
            for _ in range(half - 1):
                wait(all_v.at[0, pl.ds(0, half)], sends)

        wait(all_v.at[pl.ds(0, chips - 1)], sends)
        for c in range(CORES - 1):
            wait(all_v, sends)

    if detour:

        @pl.when(relays)
        def _():
            wait(relay_v, sends)

    @pl.when(core < CORES - 1)
    def _():
        wait(part_v, sends)

    @pl.loop(side * half, group)
    def _(_):
        wait(part_v, sends)

    with jax.named_scope("w_far"):
        wait(recv_ref.at[pl.ds(0, n - 1)], recv_a)


def write_kernel(recv_ref, att_ref, latent_out, attended_out, sem):
    copies = [
        pltpu.make_async_copy(recv_ref, latent_out, sem),
        pltpu.make_async_copy(att_ref, attended_out, sem),
    ]
    for copy in copies:
        copy.start()
    for copy in copies:
        copy.wait()


def body(grps, seqs, latent, up_key, up_value, queries, lengths, block_dest):
    groups, rank, maps = up_key.shape
    slots, block_len, width = latent.shape[1:]
    batch, q_heads, head_dim = queries.shape
    per_group = maps // head_dim
    heads = q_heads // groups
    per_kv = heads // per_group
    n = grps * seqs
    blk_seq = block_dest.shape[0] // batch
    per_seq = blk_seq // slots
    assert per_seq * slots == blk_seq and n == slots and groups == grps
    assert grps % 2 == 0 and seqs % CORES == 0 and seqs // CORES & (seqs // CORES - 1) == 0
    part_rows = heads if per_seq == 1 else 2 * heads
    anywhere = pl.BlockSpec(memory_space=pl.ANY)
    vmem = pl.BlockSpec(memory_space=pltpu.VMEM)
    dma = pltpu.SemaphoreType.DMA
    received, attended = pl.pallas_call(
        functools.partial(kernel, grps, seqs, per_seq, per_group, per_kv),
        out_shape=(
            pltpu.VMEM((n, block_len, width), latent.dtype),
            pltpu.VMEM((batch, q_heads * head_dim), jnp.float32),
        ),
        in_specs=[anywhere] * 6,
        out_specs=(vmem, vmem),
        scratch_shapes=[
            pltpu.SMEM(block_dest.shape, jnp.int32),
            pltpu.SMEM(lengths.shape, jnp.int32),
            pltpu.SMEM((n,), jnp.int32),
            pltpu.VMEM((slots, block_len, width), latent.dtype),
            pltpu.VMEM((heads, head_dim), queries.dtype),
            pltpu.VMEM((rank, maps), up_key.dtype),
            pltpu.VMEM((rank, maps), up_value.dtype),
            pltpu.VMEM((n, block_len, width), latent.dtype),
            pltpu.VMEM((block_len, width), latent.dtype),
            pltpu.VMEM((part_rows, head_dim), jnp.float32),
            pltpu.VMEM((seqs // CORES, grps, CORES, part_rows, head_dim), jnp.float32),
            dma((3,)),
            dma,
            dma((grps,)),
        ]
        + [dma] * 3
        + [pltpu.SemaphoreType.REGULAR] * 6,
        compiler_params=pltpu.CompilerParams(collective_id=0, has_side_effects=True),
        name="exchange",
    )(block_dest, lengths, latent, queries, up_key, up_value)
    decode_latent, attended = pl.pallas_call(
        write_kernel,
        out_shape=(
            jax.ShapeDtypeStruct(received.shape, received.dtype),
            jax.ShapeDtypeStruct(attended.shape, attended.dtype),
        ),
        in_specs=[anywhere] * 2,
        out_specs=(anywhere, anywhere),
        scratch_shapes=[dma],
        name="write_out",
    )(pltpu.with_memory_space_constraint(received, pltpu.VMEM), pltpu.with_memory_space_constraint(attended, pltpu.VMEM))
    return (decode_latent.reshape(1, groups, seqs, block_len, width), attended)


def solution(mesh):
    return jax.shard_map(
        functools.partial(body, mesh.shape["grp"], mesh.shape["seq"]),
        mesh=mesh,
        in_specs=(P("grp", "seq", None, None), P(), P(), P(), P(), P()),
        out_specs=(P(("grp", "seq"), None, None, None, None), P()),
        check_vma=False,
    )
```

```python
import functools
import math

import jax
import jax.numpy as jnp
from jax import lax
from jax.experimental import pallas as pl
from jax.experimental.pallas import tpu as pltpu
from jax.sharding import PartitionSpec as P

MESH = pl.DeviceIdType.MESH
CORES = 2


def pieces(x, count):
    parts = []
    for _ in range(count - 1):
        part = x.astype(jnp.bfloat16)
        parts.append(part)
        x = x - part.astype(jnp.float32)
    parts.append(x.astype(jnp.bfloat16))
    return jnp.concatenate(parts, axis=0)


def dot_pieces(x, y, dims, count):
    rows = x.shape[0]
    out = lax.dot_general(pieces(x, count), y, (dims, ((), ())), preferred_element_type=jnp.float32)
    total = out[(count - 1) * rows :]
    for k in range(count - 2, -1, -1):
        total = total + out[k * rows : (k + 1) * rows]
    return total


def attend(per_group, per_kv, left, scale, lat, q, uk, uv):
    slots, block_len, width = lat.shape
    rank = width // 2
    heads, head_dim = q.shape
    tokens = slots * block_len
    query = q[...]

    def cols(m, k):
        return m[:, k * head_dim : (k + 1) * head_dim]

    def rows(m, k):
        return m[k * per_kv : (k + 1) * per_kv]

    key_map = uk[...]
    value_map = uv[...]
    absorbed = jnp.concatenate(
        [
            rows(
                lax.dot_general(query, cols(key_map, k), (((1,), (1,)), ((), ())), preferred_element_type=jnp.float32),
                k,
            )
            for k in range(per_group)
        ],
        axis=0,
    )
    key_lat = lat[:, :, :rank].reshape(tokens, rank)
    value_lat = lat[:, :, rank:].reshape(tokens, rank)
    scores = dot_pieces(absorbed, key_lat, ((1,), (1,)), 3) * scale
    live = lax.broadcasted_iota(jnp.int32, (heads, tokens), 1) < left
    scores = jnp.where(live, scores, -1e30)
    largest = jnp.max(scores, axis=1, keepdims=True)
    weights = jnp.where(live, jnp.exp(scores - largest), 0.0)
    total = jnp.sum(weights, axis=1, keepdims=True)
    some = jnp.where(total > 0.0, total, 1.0)
    mixed = dot_pieces(weights, value_lat, ((1,), (0,)), 3) / some
    values = jnp.concatenate(
        [rows(dot_pieces(mixed, cols(value_map, k), ((1,), (0,)), 3), k) for k in range(per_group)], axis=0
    )
    return values, jnp.where(total > 0.0, largest + jnp.log(some), -1e30)


def kernel(
    grps,
    seqs,
    per_seq,
    per_group,
    per_kv,
    dest_hbm,
    len_hbm,
    lat_hbm,
    q_hbm,
    uk_hbm,
    uv_hbm,
    recv_ref,
    att_ref,
    dest_s,
    len_s,
    from_s,
    lat_v,
    q_v,
    uk_v,
    uv_v,
    out_v,
    relay_v,
    part_v,
    all_v,
    in_sems,
    recv_a,
    recv_z,
    recv_p,
    recv_c,
    plane_sem,
    line_sem,
    all_sem,
    top_sem,
    mid_sem,
):
    n = grps * seqs
    chips = seqs // CORES
    half = grps // 2
    group = lax.axis_index("grp")
    shard = lax.axis_index("seq")
    me = group * seqs + shard
    spot = shard // CORES
    core = lax.rem(shard, CORES)
    side = group // half
    first_far = (1 - side) * half
    leads = core == CORES - 1
    outer = (group == 0) | (group == grps - 1)
    inner = (group > 0) & (group < grps - 1)
    last = (group == grps - 1) & (spot == chips - 1)
    bits = [lax.rem(spot // 2**b, 2) for b in range(chips.bit_length() - 1)]
    slots, block_len, width = lat_v.shape
    heads, head_dim = q_v.shape
    barrier = pltpu.get_barrier_semaphore()
    sends = in_sems.at[0]

    def signal(sem, there):
        pl.semaphore_signal(sem, inc=1, device_id=there, device_id_type=MESH)

    def send(src, dst, there, send_sem, recv_sem):
        pltpu.make_async_remote_copy(
            src_ref=src, dst_ref=dst, send_sem=send_sem, recv_sem=recv_sem, device_id=there, device_id_type=MESH
        ).start()

    def wait(some, sem):
        pltpu.make_async_copy(some, some, sem).wait()

    def bits_in(v):
        return sum(bit for b, bit in enumerate(bits) if v >> b & 1)

    def count(of):
        total = 1
        for bit in bits:
            total = total * of(bit)
        return total

    sequence = shard // per_seq
    loads = [
        (dest_hbm, dest_s),
        (lat_hbm.at[0], lat_v),
        (q_hbm.at[sequence, pl.ds(pl.multiple_of(group * heads, heads), heads)], q_v),
        (uk_hbm.at[group], uk_v),
        (uv_hbm.at[group], uv_v),
        (len_hbm, len_s),
    ]
    loads = [pltpu.make_async_copy(src, dst, in_sems.at[min(i, 2)]) for i, (src, dst) in enumerate(loads)]
    for load in loads[:2]:
        load.start()

    with jax.named_scope("sig"):
        for c in range(1, CORES):
            signal(barrier, (group, spot * CORES + lax.rem(core + c, CORES)))
        for v in range(chips):

            @pl.when(bits_in(v) == 0)
            def _():
                @pl.loop(group + (1 if v == 0 else 0), grps)
                def _(g):
                    for c in range(CORES):
                        signal(barrier, (g, (spot + v) * CORES + c))

    for load in loads[2:]:
        load.start()
    with jax.named_scope("w_bar"):
        pl.semaphore_wait(barrier, ((group + 1) * count(lambda bit: 1 + bit) - 1) * CORES + CORES - 1)

    with jax.named_scope("sig2"):
        for v in range(1, chips):

            @pl.when(bits_in(v) == bin(v).count("1"))
            def _():
                signal(plane_sem, (group, (spot - v) * CORES + core))

        @pl.when(group == half)
        def _():
            @pl.loop(0, half)
            def _(g):
                signal(line_sem, (g, shard))

        @pl.when(group == grps - 1)
        def _():
            @pl.loop(0, grps - 1)
            def _(g):
                signal(top_sem, (g, shard))

        @pl.when((group == half) & (spot == chips - 1))
        def _():
            @pl.loop(0, half * chips)
            def _(k):
                signal(mid_sem, (k // chips, lax.rem(k, chips) * CORES + core))

        @pl.when(last)
        def _():
            @pl.loop(0, grps * chips - 1)
            def _(k):
                signal(all_sem, (k // chips, lax.rem(k, chips) * CORES + core))

    with jax.named_scope("w_dest"):
        loads[0].wait()
    lanes = pl.cdiv(n, 128) * 128
    lane = lax.broadcasted_iota(jnp.int32, (1, lanes), 1)

    def place(i, held):
        return jnp.where(lane == dest_s[shard * slots + i], i, held)

    unroll = min(slots, 32)
    source = lax.fori_loop(0, slots, place, jnp.zeros((1, lanes), jnp.int32), unroll=unroll)

    def find(d, _):
        from_s[d] = jnp.sum(jnp.where(lane == d, source, 0))
        return 0

    lax.fori_loop(0, n, find, 0, unroll=unroll)
    with jax.named_scope("w_lat"):
        loads[1].wait()

    def pick(d, _):
        out_v[d] = lat_v[from_s[d]]
        return 0

    with jax.named_scope("pick"):
        lax.fori_loop(0, n, pick, 0, unroll=unroll)
        recv_ref[me] = out_v[me]

    def block(to_group, to_shard, recv_sem):
        send(out_v.at[to_group * seqs + to_shard], recv_ref.at[me], (to_group, to_shard), sends, recv_sem)

    def turn(table, k):
        if table is None:
            return lax.rem(spot + k, chips)
        return sum(
            row[k] * math.prod(bit if a >> b & 1 else 1 - bit for b, bit in enumerate(bits))
            for a, row in enumerate(table)
            if row[k]
        )

    if chips == 4:
        upper_turns = ((0, 1, 2, 3), (0, 1, 3, 2), (0, 2, 1, 3), (1, 0, 2, 3))
        lower_turns = ((0, 3, 1, 2), (1, 2, 0, 3), (2, 1, 0, 3), (3, 0, 1, 2))
    else:
        upper_turns = lower_turns = None
    ahead_own = (spot == 0) & (core < CORES - 1)
    ahead = (spot > 0) & (chips == 4)

    def far_blocks(turns, j, first, end):
        for k in range(first, end):
            to_spot = turn(turns, k)
            for c in range(CORES):
                block(first_far + j, to_spot * CORES + lax.rem(core + c, CORES), recv_a)

    detour = lower_turns is not None and half > 1
    turns_off = (group == half - 1 + side) & (spot == chips - 1) & (core == side)
    relays = (group == half - 1 + side) & (spot == 0) & (core == side)
    off_spot = lower_turns[-1][-1] if detour else 0
    off_group = first_far + half - 1

    def later_blocks():
        for j in range(1, half):
            far_blocks(lower_turns, j, 1, chips - 1)
            if not detour or j < half - 1:
                far_blocks(lower_turns, j, chips - 1, chips)
        if detour:

            @pl.when(jnp.logical_not(turns_off))
            def _():
                far_blocks(lower_turns, half - 1, chips - 1, chips)

            @pl.when(turns_off)
            def _():
                block(off_group, off_spot * CORES + 0, recv_a)

            @pl.when(relays)
            def _():
                wait(relay_v, recv_z.at[group])
                source_row = group * seqs + (chips - 1) * CORES + core
                send(relay_v, recv_ref.at[source_row], (off_group, off_spot * CORES + 1), sends, recv_a)

    def near_blocks(lowest, highest):
        @pl.loop(lowest, highest)
        def _(g):
            @pl.loop(0, seqs)
            def _(k):
                block(g, lax.rem(shard + k, seqs), recv_a)

    @pl.when(side == 1)
    def _():
        far_blocks(upper_turns, 0, 0, 1)

        @pl.when(ahead)
        def _():
            far_blocks(upper_turns, 0, 1, 2)

        @pl.when(ahead_own)
        def _():
            for j in range(1, half):
                far_blocks(lower_turns, j, 0, 1)

    for load in loads[2:]:
        load.wait()
    with jax.named_scope("attend"):
        left = len_s[sequence] - (shard - sequence * per_seq) * (slots * block_len)
        values, size = attend(per_group, per_kv, left, 1.0 / float(head_dim) ** 0.5, lat_v, q_v, uk_v, uv_v)
        part_v[0:heads, :] = values
        if per_seq > 1:
            part_v[heads : 2 * heads, :] = jnp.broadcast_to(size, (heads, head_dim))

    @pl.loop(side * half, group)
    def _(g):
        send(part_v, all_v.at[spot, group, core], (g, spot * CORES + CORES - 1), sends, recv_z.at[group])

    @pl.when(core < CORES - 1)
    def _():
        send(part_v, all_v.at[spot, group, core], (group, spot * CORES + CORES - 1), sends, recv_c)

    @pl.when(leads)
    def _():
        all_v[spot, group, core] = part_v[...]

    @pl.when(side == 0)
    def _():
        with jax.named_scope("w_line"):
            pl.semaphore_wait(line_sem, 1)
        far_blocks(lower_turns, 0, 0, 1)

    with jax.named_scope("w_plane"):

        @pl.when(spot < chips - 1)
        def _():
            pl.semaphore_wait(plane_sem, count(lambda bit: 2 - bit) - 1)

    if detour:

        @pl.when(turns_off)
        def _():
            held = out_v.at[off_group * seqs + off_spot * CORES + 1]
            send(held, relay_v, (group, core), sends, recv_z.at[group])

    @pl.loop(1, seqs)
    def _(k):
        block(group, lax.rem(shard + k, seqs), recv_a)

    def along_line(g):
        both = all_v.at[spot, group]
        send(both, both, (g, shard), sends, recv_z.at[group])

    def over_plane(g):
        both = all_v.at[spot, g]
        for k in range(1, chips):
            send(both, both, (group, lax.rem(spot + k, chips) * CORES + core), sends, recv_p)

    def release():
        @pl.when(leads)
        def _():
            over_plane(group)

    @pl.when(core < CORES - 1)
    def _():
        near_blocks(side * half, group)

    @pl.when(leads)
    def _():
        with jax.named_scope("w_part"):
            wait(all_v.at[0, 0, pl.ds(0, CORES - 1)], recv_c)

        @pl.when(side == 1)
        def _():
            along_line(0)

        near_blocks(side * half, group)

    def parts_up():
        with jax.named_scope("w_top"):

            @pl.when(group < grps - 1)
            def _():
                pl.semaphore_wait(top_sem, 1)

        @pl.when(leads)
        def _():
            @pl.loop(group + 1, (side + 1) * half)
            def _(g):
                along_line(g)

            @pl.when(side == 0)
            def _():
                along_line(grps - 1)

    def pass_on():
        @pl.when(leads & outer)
        def _():
            for k in range(half):
                g = first_far + k
                with jax.named_scope("w_x"):
                    wait(all_v.at[0, 0], recv_z.at[g])
                crossed = all_v.at[spot, g]
                for i in range(1, half):
                    to_group = side * half + lax.rem(group - side * half + i, half)
                    send(crossed, crossed, (to_group, shard), sends, recv_z.at[g])
                over_plane(g)

    @pl.when(side == 1)
    def _():
        release()
        pass_on()

        @pl.when(jnp.logical_not(ahead))
        def _():
            far_blocks(upper_turns, 0, 1, 2)

        far_blocks(upper_turns, 0, 2, chips)
        later_blocks()

        @pl.when(jnp.logical_not(ahead_own))
        def _():
            for j in range(1, half):
                far_blocks(lower_turns, j, 0, 1)

    @pl.when(side == 0)
    def _():
        parts_up()
        release()
        with jax.named_scope("w_mid"):
            pl.semaphore_wait(mid_sem, 1)
        near_blocks(group + 1, half)
        pass_on()
        far_blocks(lower_turns, 0, 1, chips)

    with jax.named_scope("w_all"):

        @pl.when(jnp.logical_not(last))
        def _():
            pl.semaphore_wait(all_sem, 1)

    @pl.when(side == 0)
    def _():
        later_blocks()
        for j in range(1, half):
            far_blocks(lower_turns, j, 0, 1)

    @pl.when(side == 1)
    def _():
        parts_up()
        near_blocks(group + 1, grps)


    @pl.when(leads)
    def _():
        for k in range(1, grps):
            for g in (group - k, group + k):

                @pl.when((g >= 0) & (g < grps) & (inner | ((g >= side * half) & (g < (side + 1) * half))))
                def _():
                    with jax.named_scope("w_z"):
                        wait(all_v.at[0, 0], recv_z.at[g])
                    over_plane(g)

        with jax.named_scope("w_p"):
            wait(all_v.at[pl.ds(0, chips - 1)], recv_p)
        for c in range(CORES - 1):
            send(all_v, all_v, (group, spot * CORES + c), sends, recv_c)

    @pl.when(core < CORES - 1)
    def _():
        with jax.named_scope("w_c"):
            wait(all_v, recv_c)

    batch = att_ref.shape[0]
    with jax.named_scope("att"):
        for g in range(grps):
            if per_seq == 1:
                held = all_v[:, g].reshape(batch, heads, head_dim)
            else:
                part = all_v[:, g].reshape(batch, per_seq, 2 * heads, head_dim)
                sizes = part[:, :, heads:]
                share = jnp.exp(sizes - jnp.max(sizes, axis=1, keepdims=True))
                held = jnp.sum(part[:, :, :heads] * share, axis=1) / jnp.sum(share, axis=1)
            held = jnp.swapaxes(held, 0, 1)
            for h in range(heads):
                at = (g * heads + h) * head_dim
                att_ref[:, at : at + head_dim] = held[h]

    with jax.named_scope("w_send"):
        wait(recv_ref.at[pl.ds(0, n - 1)], sends)

    @pl.when(leads)
    def _():
        @pl.loop(0, half - (group - side * half))
        def _(_):
            wait(all_v.at[0, 0], sends)


        @pl.when(outer)
        def _():
            for _ in range(half - 1):
                wait(all_v.at[0, pl.ds(0, half)], sends)

        wait(all_v.at[pl.ds(0, chips - 1)], sends)
        for c in range(CORES - 1):
            wait(all_v, sends)

    if detour:

        @pl.when(relays)
        def _():
            wait(relay_v, sends)

    @pl.when(core < CORES - 1)
    def _():
        wait(part_v, sends)

    @pl.loop(side * half, group)
    def _(_):
        wait(part_v, sends)

    with jax.named_scope("w_far"):
        wait(recv_ref.at[pl.ds(0, n - 1)], recv_a)


def write_kernel(recv_ref, att_ref, latent_out, attended_out, sem):
    copies = [
        pltpu.make_async_copy(recv_ref, latent_out, sem),
        pltpu.make_async_copy(att_ref, attended_out, sem),
    ]
    for copy in copies:
        copy.start()
    for copy in copies:
        copy.wait()


def body(grps, seqs, latent, up_key, up_value, queries, lengths, block_dest):
    groups, rank, maps = up_key.shape
    slots, block_len, width = latent.shape[1:]
    batch, q_heads, head_dim = queries.shape
    per_group = maps // head_dim
    heads = q_heads // groups
    per_kv = heads // per_group
    n = grps * seqs
    blk_seq = block_dest.shape[0] // batch
    per_seq = blk_seq // slots
    assert per_seq * slots == blk_seq and n == slots and groups == grps
    assert grps % 2 == 0 and seqs % CORES == 0 and seqs // CORES & (seqs // CORES - 1) == 0
    part_rows = heads if per_seq == 1 else 2 * heads
    anywhere = pl.BlockSpec(memory_space=pl.ANY)
    vmem = pl.BlockSpec(memory_space=pltpu.VMEM)
    dma = pltpu.SemaphoreType.DMA
    received, attended = pl.pallas_call(
        functools.partial(kernel, grps, seqs, per_seq, per_group, per_kv),
        out_shape=(
            pltpu.VMEM((n, block_len, width), latent.dtype),
            pltpu.VMEM((batch, q_heads * head_dim), jnp.float32),
        ),
        in_specs=[anywhere] * 6,
        out_specs=(vmem, vmem),
        scratch_shapes=[
            pltpu.SMEM(block_dest.shape, jnp.int32),
            pltpu.SMEM(lengths.shape, jnp.int32),
            pltpu.SMEM((n,), jnp.int32),
            pltpu.VMEM((slots, block_len, width), latent.dtype),
            pltpu.VMEM((heads, head_dim), queries.dtype),
            pltpu.VMEM((rank, maps), up_key.dtype),
            pltpu.VMEM((rank, maps), up_value.dtype),
            pltpu.VMEM((n, block_len, width), latent.dtype),
            pltpu.VMEM((block_len, width), latent.dtype),
            pltpu.VMEM((part_rows, head_dim), jnp.float32),
            pltpu.VMEM((seqs // CORES, grps, CORES, part_rows, head_dim), jnp.float32),
            dma((3,)),
            dma,
            dma((grps,)),
        ]
        + [dma] * 2
        + [pltpu.SemaphoreType.REGULAR] * 5,
        compiler_params=pltpu.CompilerParams(collective_id=0, has_side_effects=True),
        name="exchange",
    )(block_dest, lengths, latent, queries, up_key, up_value)
    decode_latent, attended = pl.pallas_call(
        write_kernel,
        out_shape=(
            jax.ShapeDtypeStruct(received.shape, received.dtype),
            jax.ShapeDtypeStruct(attended.shape, attended.dtype),
        ),
        in_specs=[anywhere] * 2,
        out_specs=(anywhere, anywhere),
        scratch_shapes=[dma],
        name="write_out",
    )(pltpu.with_memory_space_constraint(received, pltpu.VMEM), pltpu.with_memory_space_constraint(attended, pltpu.VMEM))
    return (decode_latent.reshape(1, groups, seqs, block_len, width), attended)


def solution(mesh):
    return jax.shard_map(
        functools.partial(body, mesh.shape["grp"], mesh.shape["seq"]),
        mesh=mesh,
        in_specs=(P("grp", "seq", None, None), P(), P(), P(), P(), P()),
        out_specs=(P(("grp", "seq"), None, None, None, None), P()),
        check_vma=False,
    )
```
